256 devices in a mesh: dx: 8 (over z_lo, y), dy: 32 (over z_hi, x, core).
Axes of the slice: x: 4, y: 4, z: 8 (z_hi: 4, z_lo: 2; z = z_hi * 2 + z_lo), core: 2. Of those that a mesh axis runs over, the one named last changes fastest.
Arguments:
- vectors: bfloat16 [2, 64, 512, 16, 128], P(None, 'dx', 'dy'), may hold values from -6 to 6
- resident: bfloat16 [64, 512, 16, 512], P('dx', 'dy'), may hold values from -6 to 6
- inv_mass: float32 [64, 512, 16], P('dx', 'dy'), may hold values from 0.26 to 1.3
- potential: float32 [64, 512, 16], P('dx', 'dy'), may hold values from -0.4 to 0.4
- cell_matrix: bfloat16 [729, 729], replicated, may hold values from -1 to 1.3, as said below
- connectivity: int32 [8, 32, 4, 729], P('dx', 'dy'), may hold values from 0 to 2447, as said below
Outputs:
- filtered: float32 [2, 64, 512, 16, 128], P(None, 'dx', 'dy')
- margin: float32 [512, 256], P('dy')
The draws below stay inside these ranges and needn't reach their ends.
Inputs may be any that keep to these rules, and one draw needn't show every extreme that they name: `connectivity`: cell c of a device, with c = (cx * 2 + cy) * 2 + cz, covers the extended nodes with i from cx * 8 to cx * 8 + 8, j from cy * 8 to cy * 8 + 8, and k from cz * 8 to cz * 8 + 8 taken modulo 2 * 8; its 729 entries name each of these nodes once, in an order that may differ from cell to cell. `cell_matrix`: Symmetric.
All inputs are finite; a program needn't handle non-finite values.
Results may differ from the reference program's by a relative error of at most 0.0055.
Values may be sent and summed in bfloat16 or wider, within the bound.
A program may use at most 64 MiB of HBM per device.

```python
import jax
import jax.numpy as jnp
from jax import lax

P_SIZE = 8
NC = 729
CELL_X = 1
CELL_Y = 2
CELL_Z = 2
CELLS_DEV = 4
V = 128
BLOCKS = 2
RES = 512
DEGREE = 3
NX = 64
NY = 512
NZ = 16
N_DX = 8
N_DY = 32


def draw_connectivity(key, part):
    orders = jnp.array([[0, 1, 2], [0, 2, 1], [1, 0, 2], [1, 2, 0], [2, 0, 1], [2, 1, 0]], jnp.int32)
    key_order, key_flip = jax.random.split(jax.random.fold_in(key, 11))
    shape = (N_DX, N_DY, CELLS_DEV)
    which = jax.random.randint(key_order, shape, 0, 6)
    flips = jax.random.randint(key_flip, shape + (3,), 0, 2)
    local = jnp.arange(NC, dtype=jnp.int32)
    coords = jnp.stack([local // ((P_SIZE + 1) * (P_SIZE + 1)), local // (P_SIZE + 1) % (P_SIZE + 1), local % (P_SIZE + 1)], axis=-1)
    chosen = orders[which]
    onehot = (chosen[..., :, None] == jnp.arange(3, dtype=jnp.int32)).astype(jnp.int32)
    moved = jnp.sum(coords[None, None, None, :, None, :] * onehot[..., None, :, :], axis=-1)
    moved = jnp.where(flips[..., None, :] == 1, P_SIZE - moved, moved)
    cell = jnp.arange(CELLS_DEV, dtype=jnp.int32)
    cell_x = cell // (CELL_Y * CELL_Z)
    cell_y = cell // CELL_Z % CELL_Y
    cell_z = cell % CELL_Z
    index_i = cell_x[:, None] * P_SIZE + moved[..., 0]
    index_j = cell_y[:, None] * P_SIZE + moved[..., 1]
    index_k = (cell_z[:, None] * P_SIZE + moved[..., 2]) % (CELL_Z * P_SIZE)
    return ((index_i * (CELL_Y * P_SIZE + 1) + index_j) * (CELL_Z * P_SIZE) + index_k).astype(jnp.int32)


def draw_inv_mass(key, part):
    key = jax.random.fold_in(key, 23)
    edge_x = (jnp.arange(NX) % P_SIZE == 0).astype(jnp.float32)
    edge_y = (jnp.arange(NY) % P_SIZE == 0).astype(jnp.float32)
    edge_z = (jnp.arange(NZ) % P_SIZE == 0).astype(jnp.float32)
    shared = edge_x[:, None, None] + edge_y[None, :, None] + edge_z[None, None, :]
    multiple = jnp.exp2(shared)
    factor = jnp.exp(jax.random.uniform(key, (NX, NY, NZ), jnp.float32, jnp.log(0.75), jnp.log(1.3)))
    return (factor / jnp.sqrt(multiple)).astype(jnp.float32)


def draw_cell_matrix(key, part):
    key_off, key_diag = jax.random.split(jax.random.fold_in(key, 37))
    raw = jax.random.normal(key_off, (NC, NC), jnp.float32)
    offdiag = (raw + raw.T) * (0.6 / jnp.sqrt(2.0 * NC))
    offdiag = jnp.clip(offdiag, -0.3, 0.3)
    diagonal = jax.random.uniform(key_diag, (NC,), jnp.float32, 0.8, 1.2)
    whole = offdiag * (1.0 - jnp.eye(NC, dtype=jnp.float32)) + jnp.diag(diagonal)
    return whole.astype(jnp.bfloat16)


def with_spikes(drawn, stream_key, source, target, shards_of, factor):
    owner, partner = [(jnp.arange(drawn.shape[dim]) // (drawn.shape[dim] // shards_of)).reshape([-1 if axis == dim else 1 for axis in range(drawn.ndim)]) for dim in (source, target)]
    chosen = jax.random.permutation(stream_key, shards_of)[partner]
    strong = (owner == chosen) | (owner == (partner + shards_of // 2) % shards_of)
    return jnp.where(strong, factor * drawn, drawn)


def level_of(own_key, dims, shards, low, high):
    level, own = 1.0, jax.random.fold_in(own_key, 6)
    for position, parts in shards:
        steps = jnp.exp(jax.random.uniform(jax.random.fold_in(own, position), (parts,), jnp.float32, low / len(shards), high / len(shards)))
        level = level * jnp.repeat(steps, dims[position] // parts).reshape([-1 if axis == position else 1 for axis in range(len(dims))])
    return level


def normal_values(own_key, shape, width, bound, cuts=(), kind=jnp.bfloat16):
    values = width * jax.random.normal(own_key, shape, jnp.float32)
    if cuts:
        values = values * level_of(own_key, shape, cuts, -0.22, 0.18)
    return jnp.clip(values, -bound, bound).astype(kind)


def heavy_noise(rng, shape, deviation, limit, shards, heavy, held_as=jnp.bfloat16):
    result = deviation * jax.random.normal(rng, shape, jnp.float32)
    if shards:
        result = result * level_of(rng, shape, shards, -0.22, 0.18)
    return jnp.clip(with_spikes(result, jax.random.fold_in(rng, 3), *heavy), -limit, limit).astype(held_as)


def setup_inputs(seed: int = 0) -> dict:
    splits = jax.random.split(jax.random.key(seed), 7)
    vectors = normal_values(splits[0], (BLOCKS, NX, NY, NZ, V), 1.0, 6.0, ((1, 8), (2, 32)))
    resident = heavy_noise(splits[1], (NX, NY, NZ, RES), 1.0, 6.0, ((0, 8), (1, 32)), (1, 3, 32, 2.75))
    inv_mass = draw_inv_mass(jax.random.fold_in(splits[6], 71), 0)
    potential = jnp.clip(jax.random.uniform(splits[3], (NX, NY, NZ), jnp.float32, -0.4, 0.4) * level_of(splits[3], (NX, NY, NZ), ((0, 8), (1, 32)), -0.4, 0.0), -0.4, 0.4)
    cell_matrix = draw_cell_matrix(jax.random.fold_in(splits[6], 71), 0)
    connectivity = draw_connectivity(jax.random.fold_in(splits[6], 71), 0)
    return {"vectors": vectors, "resident": resident, "inv_mass": inv_mass, "potential": potential, "cell_matrix": cell_matrix, "connectivity": connectivity}


center_shift = 1.2
half_width = 2.0

def node_table(connectivity):
    count_x, count_y, cell_count, node_count = connectivity.shape
    ext_y = CELL_Y * P_SIZE + 1
    ext_z = CELL_Z * P_SIZE
    index_i = connectivity // (ext_y * ext_z)
    index_j = connectivity // ext_z % ext_y
    index_k = connectivity % ext_z
    place_x = jnp.arange(count_x, dtype=jnp.int32)[:, None, None, None]
    place_y = jnp.arange(count_y, dtype=jnp.int32)[None, :, None, None]
    global_x = (place_x * (CELL_X * P_SIZE) + index_i) % NX
    global_y = (place_y * (CELL_Y * P_SIZE) + index_j) % NY
    flat = (global_x * NY + global_y) * NZ + index_k
    return flat.reshape(count_x * count_y, cell_count * node_count).astype(jnp.int32)

def apply_hamiltonian(values, inv_mass, potential, cell_matrix, table):
    vec_width = values.shape[-1]
    scaled = (values * inv_mass[..., None]).astype(jnp.bfloat16).reshape(-1, vec_width)
    kinetic = cell_matrix.astype(jnp.float32)

    def add_domain(total, indices):
        picked = scaled[indices].astype(jnp.float32).reshape(CELLS_DEV, NC, vec_width)
        product = jnp.einsum('il,clw->ciw', kinetic, picked, precision=lax.Precision.HIGHEST)
        return (total.at[indices].add(product.reshape(-1, vec_width)), None)
    start = jnp.zeros((NX * NY * NZ, vec_width), jnp.float32)
    total, unused = lax.scan(add_domain, start, table)
    assembled = total.reshape(values.shape)
    return inv_mass[..., None] * assembled + potential[..., None] * values

def reference(vectors, resident, inv_mass, potential, cell_matrix, connectivity):
    table = node_table(connectivity)
    resident_rows = resident.reshape(-1, RES)
    norm_scale = 1.0 / jnp.sqrt(jnp.float32(NX * NY * NZ))
    results = []
    margins = []
    for block_id in range(BLOCKS):
        start = vectors[block_id].astype(jnp.float32)
        image = apply_hamiltonian(start, inv_mass, potential, cell_matrix, table)
        older = start
        current = (image - center_shift * start) / half_width
        for degree_id in range(1, DEGREE):
            image = apply_hamiltonian(current, inv_mass, potential, cell_matrix, table)
            newer = 2.0 * (image - center_shift * current) / half_width - older
            older = current
            current = newer
        results.append(current)
        rounded = current.astype(jnp.bfloat16).reshape(-1, V)
        inner = lax.dot_general(resident_rows, rounded, (((0,), (0,)), ((), ())), preferred_element_type=jnp.float32)
        margins.append(inner * norm_scale)
    return (jnp.stack(results), jnp.concatenate(margins, axis=1))
```

```python
import math

import jax
import jax.numpy as jnp
from jax import lax
from jax.experimental import pallas as pl
from jax.experimental.pallas import tpu as pltpu
from jax.sharding import PartitionSpec as P

MESH = pl.DeviceIdType.MESH
BLOCKS = 2
DEGREE = 3
NCELL = 4
KP = 768
LO, EX, EY, EZ = 8, 9, 17, 16
W = 128
center_shift = 1.2
half_width = 2.0
ZL, NYC = 2, 4
ZH, NXC, CORES = 4, 4, 2
F32, BF16 = jnp.float32, jnp.bfloat16


def kernel(
    norm_scale, vec, res, coef, pos, amat, out, margin,
    ac, acc, uf, y, im, bt, ub, wp, mloc,
    xh, yh, dh, cx, cy_, cd, sx, sy, rx, ry, rd,
    m1s, m1r, m2s, m2r, m3s, m3r, m4s, m4r,
    hs_sem, hr_sem, es_sem, er_sem, s1, r1, s2, r2, s3, r3, s4, r4, osem,
):
    p = lax.axis_index("dx")
    q = lax.axis_index("dy")
    ndx, ndy = ZL * NYC, ZH * NXC * CORES
    zl, yc = p // NYC, p % NYC
    core, xc, zh = q % CORES, (q // CORES) % NXC, q // (CORES * NXC)
    pm, pp = (p + ndx - 1) % ndx, (p + 1) % ndx
    qm, qp = (q + ndy - 1) % ndy, (q + 1) % ndy

    def dy_of(zhv, xv, cv):
        return (zhv * NXC + xv) * CORES + cv

    neighbours = [(pm, q), (pp, q), (p, qm), (p, qp), (pm, qm), (pp, qp), (pm, qp), (pp, qm)]
    partner = [(p, dy_of(zh, xc, CORES - 1 - core))]
    row = [(p, dy_of(zh, (xc + k) % NXC, core)) for k in range(1, NXC)]
    nz = ZL * ZH
    zi = zh * ZL + zl
    column = []
    for k in range(1, nz):
        other = (zi + k) % nz
        column.append(((other % ZL) * NYC + yc, dy_of(other // ZL, xc, core)))
    group = [((p + k) % ndx, q) for k in range(1, ndx)]

    barrier = pltpu.get_barrier_semaphore()
    greeted = neighbours + partner + row + column + group
    for device in greeted:
        pl.semaphore_signal(barrier, inc=1, device_id=device, device_id_type=MESH)
    pl.semaphore_wait(barrier, len(greeted))

    def remote(src, dst, ssem, rsem, device):
        return pltpu.make_async_remote_copy(
            src_ref=src, dst_ref=dst, send_sem=ssem, recv_sem=rsem, device_id=device, device_id_type=MESH
        )

    halo = [
        remote(vec.at[:, 0], xh, hs_sem.at[0], hr_sem.at[0], (pm, q)),
        remote(vec.at[:, :, 0], yh, hs_sem.at[1], hr_sem.at[1], (p, qm)),
        remote(vec.at[:, 0, 0], dh, hs_sem.at[2], hr_sem.at[2], (pm, qm)),
        remote(coef.at[0], cx, hs_sem.at[3], hr_sem.at[3], (pm, q)),
        remote(coef.at[LO], cy_, hs_sem.at[4], hr_sem.at[4], (p, qm)),
        remote(coef.at[0], cd, hs_sem.at[5], hr_sem.at[5], (pm, qm)),
    ]
    for copy in halo:
        copy.start()

    def spread(tile, lane):
        return jnp.broadcast_to(tile[:, lane : lane + 1], (EZ, W))

    def coefs(i, j, mass, pot):
        im[i, j] = mass
        bt[i, j] = (pot - center_shift) * (1.0 / half_width)

    def begin(i, j, values):
        for b in range(BLOCKS):
            value = values[b].astype(F32)
            y[0, b, i, j] = value
            uf[b, i, j] = value * im[i, j]

    def fill(i, carry):
        tile = coef[i]
        for j in range(EZ):
            coefs(i, j, spread(tile, j), spread(tile, EZ + j))
        for b in range(BLOCKS):
            value = vec[b, i].astype(F32)
            y[0, b, i, 0:16] = value
            uf[b, i, 0:16] = value * im[i, 0:16]
        return carry

    lax.fori_loop(0, LO, fill, 0)
    y[1] = jnp.zeros_like(y[1])

    def permute(c, carry):
        place = pos[c]
        onehot = (lax.broadcasted_iota(jnp.int32, (KP, KP), 0) == place).astype(F32).astype(BF16)
        rows = jnp.dot(onehot, amat[...], preferred_element_type=F32).astype(BF16)
        ac[c] = lax.dot_general(rows, onehot, (((1,), (1,)), ((), ())), preferred_element_type=F32).astype(BF16)
        return carry

    lax.fori_loop(0, NCELL, permute, 0)

    for copy in halo:
        copy.wait()
    tile = cx[...]
    for j in range(EZ):
        coefs(LO, j, spread(tile, j), spread(tile, EZ + j))
    tile = cy_[...]
    for i in range(LO):
        coefs(i, 16, spread(tile, i), spread(tile, LO + i))
    tile = cd[...]
    coefs(LO, 16, spread(tile, 0), spread(tile, EZ))
    for b in range(BLOCKS):
        value = xh[b].astype(F32)
        y[0, b, LO, 0:16] = value
        uf[b, LO, 0:16] = value * im[LO, 0:16]
        value = yh[b].astype(F32)
        y[0, b, 0:LO, 16] = value
        uf[b, 0:LO, 16] = value * im[0:LO, 16]
        value = dh[b].astype(F32)
        y[0, b, LO, 16] = value
        uf[b, LO, 16] = value * im[LO, 16]

    def exchange(d):
        plan = [
            (sx.at[d, 0], rx.at[d, 1], (pm, q)),
            (sx.at[d, 1], rx.at[d, 0], (pp, q)),
            (sy.at[d, 0], ry.at[d, 1], (p, qm)),
            (sy.at[d, 1], ry.at[d, 0], (p, qp)),
            (sx.at[d, 0, :, 0], rd.at[d, 3], (pm, qm)),
            (sx.at[d, 1, :, 16], rd.at[d, 0], (pp, qp)),
            (sx.at[d, 0, :, 16], rd.at[d, 2], (pm, qp)),
            (sx.at[d, 1, :, 0], rd.at[d, 1], (pp, qm)),
        ]
        return [remote(s, t, es_sem.at[d, n], er_sem.at[d, n], to) for n, (s, t, to) in enumerate(plan)]

    def apply(d, carry):
        now, later = lax.rem(d, 2), lax.rem(d + 1, 2)
        scale = jnp.where(d == 0, 1.0, 2.0).astype(F32)
        keep = jnp.where(d == 0, 0.0, 1.0).astype(F32)
        for cy in range(2):
            for cz in range(2):
                c = cy * 2 + cz
                kp = (8 * cz + 8) % 16
                for b in range(BLOCKS):
                    flat = uf.at[b].reshape(EX * EY * EZ, W)
                    main = uf[b, :, 8 * cy : 8 * cy + 9, 8 * cz : 8 * cz + 8, :].reshape(648, W)
                    planes = [flat[pl.ds((i * EY + 8 * cy) * EZ + kp, 8, EZ), :] for i in range(EX)]
                    start = (8 * cy + 8) * EZ + kp
                    line = flat[pl.ds(start, 8, EY * EZ), :]
                    last = flat[pl.ds(start + 8 * EY * EZ, 1), :]
                    first = lax.broadcasted_iota(jnp.int32, (8, W), 0) == 0
                    last = jnp.where(first, jnp.broadcast_to(last, (8, W)), 0.0)
                    whole = jnp.concatenate([main] + planes + [line, last, jnp.zeros((32, W), F32)], axis=0)
                    ub[:, b * W : (b + 1) * W] = whole.astype(BF16)
                w = jnp.dot(ac[c], ub[...], preferred_element_type=F32)
                wp[c] = w[648:]
                for b in range(BLOCKS):
                    block = w[:648, b * W : (b + 1) * W].reshape(EX, 9, 8, W)
                    ks = slice(8 * cz, 8 * cz + 8)
                    if cy == 0:
                        acc[b, :, 0:9, ks, :] = block
                    else:
                        acc[b, :, 8, ks, :] += block[:, 0]
                        acc[b, :, 9:17, ks, :] = block[:, 1:]
        for cy in range(2):
            for cz in range(2):
                c = cy * 2 + cz
                kp = (8 * cz + 8) % 16
                for b in range(BLOCKS):
                    flat = acc.at[b].reshape(EX * EY * EZ, W)
                    cols = slice(b * W, (b + 1) * W)
                    for i in range(EX):
                        where = pl.ds((i * EY + 8 * cy) * EZ + kp, 8, EZ)
                        flat[where, :] = flat[where, :] + wp[c, 8 * i : 8 * i + 8, cols]
                    start = (8 * cy + 8) * EZ + kp
                    where = pl.ds(start, 8, EY * EZ)
                    flat[where, :] = flat[where, :] + wp[c, 72:80, cols]
                    where = pl.ds(start + 8 * EY * EZ, 1)
                    flat[where, :] = flat[where, :] + wp[c, 80:81, cols]
        for b in range(BLOCKS):
            sx[d, 0, b] = acc[b, 0].astype(BF16)
            sx[d, 1, b] = acc[b, LO].astype(BF16)
            sy[d, 0, b] = acc[b, :, 0].astype(BF16)
            sy[d, 1, b] = acc[b, :, 16].astype(BF16)
        copies = exchange(d)
        for copy in copies:
            copy.start()

        def update(b, i, j):
            mass = im[i, j]
            fresh = scale * (acc[b, i, j] * (mass * (1.0 / half_width)) + bt[i, j] * y[now, b, i, j]) - keep * y[later, b, i, j]
            y[later, b, i, j] = fresh
            uf[b, i, j] = fresh * mass

        def inner(i, carry):
            for b in range(BLOCKS):
                update(b, i, slice(1, 16))
            return carry

        lax.fori_loop(1, LO, inner, 0)
        for copy in copies:
            copy.wait()
        for b in range(BLOCKS):
            acc[b, 0] += rx[d, 0, b].astype(F32)
            acc[b, LO] += rx[d, 1, b].astype(F32)
            acc[b, :, 0] += ry[d, 0, b].astype(F32)
            acc[b, :, 16] += ry[d, 1, b].astype(F32)
            acc[b, 0, 0] += rd[d, 0, b].astype(F32)
            acc[b, 0, 16] += rd[d, 1, b].astype(F32)
            acc[b, LO, 0] += rd[d, 2, b].astype(F32)
            acc[b, LO, 16] += rd[d, 3, b].astype(F32)
        for b in range(BLOCKS):
            update(b, 0, slice(0, 17))
            update(b, LO, slice(0, 17))
            update(b, slice(1, LO), 0)
            update(b, slice(1, LO), 16)
        return carry

    lax.fori_loop(0, DEGREE, apply, 0)
    final = DEGREE % 2
    writes = [
        pltpu.make_async_copy(y.at[final, b, pl.ds(0, LO), pl.ds(0, 16)], out.at[b], osem.at[b])
        for b in range(BLOCKS)
    ]
    for copy in writes:
        copy.start()

    mloc[...] = jnp.zeros_like(mloc)

    def product(i, carry):
        cols = [y[final, b, i, 0:16].reshape(256, W).astype(BF16) for b in range(BLOCKS)]
        right = jnp.concatenate(cols, axis=1)
        left = res[i]
        mloc[...] += lax.dot_general(left, right, (((0,), (0,)), ((), ())), preferred_element_type=F32)
        return carry

    lax.fori_loop(0, LO, product, 0)

    span = CORES * 16
    for g in range(ZH * NXC):
        m1s[g] = (mloc[pl.ds(pl.multiple_of(g * span + (CORES - 1 - core) * 16, 16), 16), :] * norm_scale).astype(BF16)
    copy = remote(m1s, m1r, s1.at[0], r1.at[0], partner[0])
    copy.start()
    copy.wait()

    def both(g):
        own = mloc[pl.ds(pl.multiple_of(g * span + core * 16, 16), 16), :] * norm_scale
        return own + m1r[g].astype(F32)

    for zv in range(ZH):
        for k in range(1, NXC):
            m2s[k - 1, zv] = both(zv * NXC + (xc + k) % NXC).astype(BF16)
    copies = [remote(m2s.at[k], m2r.at[k], s2.at[k], r2.at[k], row[k]) for k in range(NXC - 1)]
    for copy in copies:
        copy.start()
    for copy in copies:
        copy.wait()
    for zv in range(ZH):
        total = both(zv * NXC + xc)
        for k in range(NXC - 1):
            total = total + m2r[k, zv].astype(F32)
        for half in range(ZL):
            m3s[zv * ZL + half] = total[half * 8 : half * 8 + 8]
    copies = [
        remote(m3s.at[(zi + k + 1) % nz], m3r.at[k], s3.at[k], r3.at[k], column[k]) for k in range(nz - 1)
    ]
    for copy in copies:
        copy.start()
    for copy in copies:
        copy.wait()
    total = m3s[zi]
    for k in range(nz - 1):
        total = total + m3r[k]
    m4s[...] = total
    m4r[p] = total
    copies = [remote(m4s, m4r.at[p], s4.at[k], r4.at[k], group[k]) for k in range(ndx - 1)]
    for copy in copies:
        copy.start()
    for copy in copies:
        copy.wait()
    for half in range(ZL):
        total = m4r[half * NYC]
        for k in range(1, NYC):
            total = total + m4r[half * NYC + k]
        margin[half * 8 : half * 8 + 8, :] = total
    for copy in writes:
        copy.wait()


def places(connectivity):
    index = connectivity.reshape(NCELL, -1)
    cell = jnp.arange(NCELL, dtype=jnp.int32)[:, None]
    cy, cz = cell // 2, cell % 2
    i = index // (EY * EZ)
    j = index // EZ % EY - 8 * cy
    k = index % EZ
    inside = k // 8 == cz
    plane = jnp.where(j < 8, 648 + i * 8 + j, 720 + i)
    where = jnp.where(inside, (i * 9 + j) * 8 + k % 8, plane)
    where = jnp.pad(where, ((0, 0), (0, KP - where.shape[1])), constant_values=-1)
    return where.reshape(NCELL, 1, KP)


def body(vectors, resident, inv_mass, potential, cell_matrix, connectivity):
    total_nodes = inv_mass.size * lax.axis_size("dx") * lax.axis_size("dy")
    norm_scale = 1.0 / math.sqrt(total_nodes)
    pos = places(connectivity)
    nc = cell_matrix.shape[0]
    amat = jnp.pad(cell_matrix, ((0, KP - nc), (0, KP - nc)))
    both = jnp.concatenate([inv_mass.transpose(0, 2, 1), potential.transpose(0, 2, 1)], axis=-1)
    edge = jnp.concatenate([inv_mass[:, 0].T, potential[:, 0].T], axis=-1)
    coef = jnp.concatenate(
        [jnp.pad(both, ((0, 0), (0, 0), (0, W - 32))), jnp.pad(edge, ((0, 0), (0, W - 16)))[None]], axis=0
    )
    res = resident.reshape(LO, 256, resident.shape[-1])
    ndx, ndy = ZL * NYC, ZH * NXC * CORES
    nz = ZL * ZH
    rows = 16 * ndy
    vmem = pl.BlockSpec(memory_space=pltpu.VMEM)
    dma = pltpu.SemaphoreType.DMA

    def k(*refs):
        kernel(norm_scale, *refs)

    state = (BLOCKS, EX, EY, EZ, W)
    return pl.pallas_call(
        k,
        out_shape=(
            jax.ShapeDtypeStruct((BLOCKS, LO, 16, EZ, W), F32),
            jax.ShapeDtypeStruct((16, BLOCKS * W), F32),
        ),
        in_specs=[vmem] * 5,
        out_specs=(pl.BlockSpec(memory_space=pl.ANY), vmem),
        scratch_shapes=[
            pltpu.VMEM((NCELL, KP, KP), BF16),
            pltpu.VMEM(state, F32),
            pltpu.VMEM(state, F32),
            pltpu.VMEM((2, *state), F32),
            pltpu.VMEM((EX, EY, EZ, W), F32),
            pltpu.VMEM((EX, EY, EZ, W), F32),
            pltpu.VMEM((KP, BLOCKS * W), BF16),
            pltpu.VMEM((NCELL, KP - 648, BLOCKS * W), F32),
            pltpu.VMEM((rows, BLOCKS * W), F32),
            pltpu.VMEM((BLOCKS, 16, EZ, W), BF16),
            pltpu.VMEM((BLOCKS, LO, EZ, W), BF16),
            pltpu.VMEM((BLOCKS, EZ, W), BF16),
            pltpu.VMEM((EZ, W), F32),
            pltpu.VMEM((EZ, W), F32),
            pltpu.VMEM((EZ, W), F32),
            pltpu.VMEM((DEGREE, 2, BLOCKS, EY, EZ, W), BF16),
            pltpu.VMEM((DEGREE, 2, BLOCKS, EX, EZ, W), BF16),
            pltpu.VMEM((DEGREE, 2, BLOCKS, EY, EZ, W), BF16),
            pltpu.VMEM((DEGREE, 2, BLOCKS, EX, EZ, W), BF16),
            pltpu.VMEM((DEGREE, 4, BLOCKS, EZ, W), BF16),
            pltpu.VMEM((ZH * NXC, 16, BLOCKS * W), BF16),
            pltpu.VMEM((ZH * NXC, 16, BLOCKS * W), BF16),
            pltpu.VMEM((NXC - 1, ZH, 16, BLOCKS * W), BF16),
            pltpu.VMEM((NXC - 1, ZH, 16, BLOCKS * W), BF16),
            pltpu.VMEM((nz, 8, BLOCKS * W), F32),
            pltpu.VMEM((nz - 1, 8, BLOCKS * W), F32),
            pltpu.VMEM((8, BLOCKS * W), F32),
            pltpu.VMEM((ndx, 8, BLOCKS * W), F32),
            dma((6,)), dma((6,)), dma((DEGREE, 8)), dma((DEGREE, 8)),
            dma((1,)), dma((1,)), dma((NXC - 1,)), dma((NXC - 1,)),
            dma((nz - 1,)), dma((nz - 1,)), dma((ndx - 1,)), dma((ndx - 1,)), dma((BLOCKS,)),
        ],
        compiler_params=pltpu.CompilerParams(
            collective_id=0, has_side_effects=True, vmem_limit_bytes=60 * 1024 * 1024
        ),
    )(vectors, res, coef, pos, amat)


def solution(mesh):
    return jax.shard_map(
        body,
        mesh=mesh,
        in_specs=(
            P(None, "dx", "dy", None, None),
            P("dx", "dy", None, None),
            P("dx", "dy", None),
            P("dx", "dy", None),
            P(),
            P("dx", "dy", None, None),
        ),
        out_specs=(P(None, "dx", "dy", None, None), P("dy", None)),
        check_vma=False,
    )
```

```python
import math

import jax
import jax.numpy as jnp
from jax import lax
from jax.experimental import pallas as pl
from jax.experimental.pallas import tpu as pltpu
from jax.sharding import PartitionSpec as P

MESH = pl.DeviceIdType.MESH
BLOCKS = 2
DEGREE = 3
NCELL = 4
KP = 768
LO, EX, EY, EZ = 8, 9, 17, 16
W = 128
center_shift = 1.2
half_width = 2.0
ZL, NYC = 2, 4
ZH, NXC, CORES = 4, 4, 2
F32, BF16 = jnp.float32, jnp.bfloat16


def kernel(
    norm_scale, vec, res, mass, pot, amat, conn, out, margin,
    ap, ac, acc, uf, y, im, bt, ub, wp, mloc, rs, posr, ct,
    xh, yh, dh, cx, cy_, cd, sx, sy, rx, ry, rd,
    m1s, m1r, m2s, m2r, m3s, m3r, m4s, m4r,
    hs_sem, hr_sem, es_sem, er_sem, s1, r1, s2, r2, s3, r3, s4, r4, osem, lsem,
):
    p = lax.axis_index("dx")
    q = lax.axis_index("dy")
    ndx, ndy = ZL * NYC, ZH * NXC * CORES
    zl, yc = p // NYC, p % NYC
    core, xc, zh = q % CORES, (q // CORES) % NXC, q // (CORES * NXC)
    pm, pp = (p + ndx - 1) % ndx, (p + 1) % ndx
    qm, qp = (q + ndy - 1) % ndy, (q + 1) % ndy

    def dy_of(zhv, xv, cv):
        return (zhv * NXC + xv) * CORES + cv

    neighbours = [(pm, q), (pp, q), (p, qm), (p, qp), (pm, qm), (pp, qp), (pm, qp), (pp, qm)]
    partner = [(p, dy_of(zh, xc, CORES - 1 - core))]
    row = [(p, dy_of(zh, (xc + k) % NXC, core)) for k in range(1, NXC)]
    nz = ZL * ZH
    zi = zh * ZL + zl
    column = []
    for k in range(1, nz):
        other = (zi + k) % nz
        column.append(((other % ZL) * NYC + yc, dy_of(other // ZL, xc, core)))
    group = [((p + k) % ndx, q) for k in range(1, ndx)]

    barrier = pltpu.get_barrier_semaphore()
    greeted = neighbours + partner + row + column + group
    for device in greeted:
        pl.semaphore_signal(barrier, inc=1, device_id=device, device_id_type=MESH)
    load = pltpu.make_async_copy(res, rs.at[pl.ds(0, LO), pl.ds(0, 16)], lsem.at[0])
    load.start()

    def remote(src, dst, ssem, rsem, device):
        return pltpu.make_async_remote_copy(
            src_ref=src, dst_ref=dst, send_sem=ssem, recv_sem=rsem, device_id=device, device_id_type=MESH
        )

    ct[0] = mass[...].reshape(LO * 16, EZ).T
    ct[1] = pot[...].reshape(LO * 16, EZ).T

    index = conn[0, 0]
    cell = lax.broadcasted_iota(jnp.int32, index.shape, 0)
    k = index & 15
    t = index >> 4
    i = (t * 241) >> 12
    j = t - i * EY - 8 * (cell >> 1)
    inside = (k >> 3) == (cell & 1)
    plane = jnp.where(j < 8, 648 + i * 8 + j, 720 + i)
    where = jnp.where(inside, (i * 9 + j) * 8 + (k & 7), plane)
    posr[...] = jnp.full(posr.shape, -1, jnp.int32)
    nc = index.shape[1]
    for c in range(NCELL):
        posr[c, :, 0:nc] = where[c : c + 1]
    ap[...] = jnp.zeros_like(ap)
    ap[0:nc, 0:nc] = amat[...]

    def spread(tile, lane):
        return jnp.broadcast_to(tile[:, lane : lane + 1], (EZ, W))

    def coefs(i, j, mass_ij, pot_ij):
        im[i, j] = mass_ij
        bt[i, j] = (pot_ij - center_shift) * (1.0 / half_width)

    for i in range(LO):
        for j in range(16):
            coefs(i, j, spread(ct[0], i * 16 + j), spread(ct[1], i * 16 + j))

    def permute(c, carry):
        onehot = (lax.broadcasted_iota(jnp.int32, (KP, KP), 0) == posr[c]).astype(F32).astype(BF16)
        rows = jnp.dot(onehot, ap[...], preferred_element_type=F32).astype(BF16)
        ac[c] = lax.dot_general(rows, onehot, (((1,), (1,)), ((), ())), preferred_element_type=F32).astype(BF16)
        return carry

    lax.fori_loop(0, 1, permute, 0)

    pl.semaphore_wait(barrier, len(greeted))
    halo = [
        remote(ct, cd, hs_sem.at[5], hr_sem.at[5], (pm, qm)),
        remote(vec.at[:, 0, 0], dh, hs_sem.at[2], hr_sem.at[2], (pm, qm)),
        remote(ct, cx, hs_sem.at[3], hr_sem.at[3], (pm, q)),
        remote(ct, cy_, hs_sem.at[4], hr_sem.at[4], (p, qm)),
        remote(vec.at[:, 0], xh, hs_sem.at[0], hr_sem.at[0], (pm, q)),
        remote(vec.at[:, :, 0], yh, hs_sem.at[1], hr_sem.at[1], (p, qm)),
    ]
    for copy in halo:
        copy.start()
    rhalo = [
        remote(res.at[0], rs.at[LO, pl.ds(0, 16)], hs_sem.at[6], hr_sem.at[6], (pm, q)),
        remote(res.at[:, 0], rs.at[pl.ds(0, LO), 16], hs_sem.at[7], hr_sem.at[7], (p, qm)),
        remote(res.at[0, 0], rs.at[LO, 16], hs_sem.at[8], hr_sem.at[8], (pm, qm)),
    ]
    for copy in rhalo:
        copy.start()

    def fill(i, carry):
        for b in range(BLOCKS):
            value = vec[b, i].astype(F32)
            y[0, b, i, 0:16] = value
            uf[b, i, 0:16] = value * im[i, 0:16]
        return carry

    lax.fori_loop(0, LO, fill, 0)
    y[1] = jnp.zeros_like(y[1])
    lax.fori_loop(1, NCELL, permute, 0)

    for copy in halo:
        copy.wait()
    for j in range(16):
        coefs(LO, j, spread(cx[0], j), spread(cx[1], j))
    for i in range(LO):
        coefs(i, 16, spread(cy_[0], i * 16), spread(cy_[1], i * 16))
    coefs(LO, 16, spread(cd[0], 0), spread(cd[1], 0))
    for b in range(BLOCKS):
        value = xh[b].astype(F32)
        y[0, b, LO, 0:16] = value
        uf[b, LO, 0:16] = value * im[LO, 0:16]
        value = yh[b].astype(F32)
        y[0, b, 0:LO, 16] = value
        uf[b, 0:LO, 16] = value * im[0:LO, 16]
        value = dh[b].astype(F32)
        y[0, b, LO, 16] = value
        uf[b, LO, 16] = value * im[LO, 16]

    low, high = pl.ds(0, 8), pl.ds(8, 9)

    def exchange(d, part):
        if part == 0:
            plan = [
                (0, sx.at[d, 0, :, low], rx.at[d, 1, :, low], (pm, q)),
                (1, sx.at[d, 1, :, low], rx.at[d, 0, :, low], (pp, q)),
                (2, sy.at[d, 0], ry.at[d, 1], (p, qm)),
                (4, sx.at[d, 0, :, 0], rd.at[d, 3], (pm, qm)),
                (7, sx.at[d, 1, :, 0], rd.at[d, 1], (pp, qm)),
            ]
            wanted = (1,)
        else:
            plan = [
                (8, sx.at[d, 0, :, high], rx.at[d, 1, :, high], (pm, q)),
                (9, sx.at[d, 1, :, high], rx.at[d, 0, :, high], (pp, q)),
                (3, sy.at[d, 1], ry.at[d, 0], (p, qp)),
                (5, sx.at[d, 1, :, 16], rd.at[d, 0], (pp, qp)),
                (6, sx.at[d, 0, :, 16], rd.at[d, 2], (pm, qp)),
            ]
            wanted = (9, 3, 5)
        last = isinstance(d, int) and d == DEGREE - 1
        return [
            remote(s, t, es_sem.at[d, n], er_sem.at[d, n], to) for n, s, t, to in plan if n in wanted or not last
        ]

    def cells(d, cy):
        for cz in range(2):
            c = cy * 2 + cz
            kp = (8 * cz + 8) % 16
            for b in range(BLOCKS):
                flat = uf.at[b].reshape(EX * EY * EZ, W)
                main = uf[b, :, 8 * cy : 8 * cy + 9, 8 * cz : 8 * cz + 8, :].reshape(648, W)
                planes = [flat[pl.ds((i * EY + 8 * cy) * EZ + kp, 8, EZ), :] for i in range(EX)]
                start = (8 * cy + 8) * EZ + kp
                line = flat[pl.ds(start, 8, EY * EZ), :]
                last = flat[pl.ds(start + 8 * EY * EZ, 1), :]
                first = lax.broadcasted_iota(jnp.int32, (8, W), 0) == 0
                last = jnp.where(first, jnp.broadcast_to(last, (8, W)), 0.0)
                whole = jnp.concatenate([main] + planes + [line, last, jnp.zeros((32, W), F32)], axis=0)
                ub[c, :, b * W : (b + 1) * W] = whole.astype(BF16)
            w = jnp.dot(ac[c], ub[c], preferred_element_type=F32)
            wp[c] = w[648:]
            for b in range(BLOCKS):
                block = w[:648, b * W : (b + 1) * W].reshape(EX, 9, 8, W)
                ks = slice(8 * cz, 8 * cz + 8)
                if cy == 0:
                    acc[b, :, 0:9, ks, :] = block
                else:
                    acc[b, :, 8, ks, :] += block[:, 0]
                    acc[b, :, 9:17, ks, :] = block[:, 1:]
        for cz in range(2):
            c = cy * 2 + cz
            kp = (8 * cz + 8) % 16
            for b in range(BLOCKS):
                flat = acc.at[b].reshape(EX * EY * EZ, W)
                cols = slice(b * W, (b + 1) * W)
                for i in range(EX):
                    where = pl.ds((i * EY + 8 * cy) * EZ + kp, 8, EZ)
                    flat[where, :] = flat[where, :] + wp[c, 8 * i : 8 * i + 8, cols]
                start = (8 * cy + 8) * EZ + kp
                where = pl.ds(start, 8, EY * EZ)
                flat[where, :] = flat[where, :] + wp[c, 72:80, cols]
                where = pl.ds(start + 8 * EY * EZ, 1)
                flat[where, :] = flat[where, :] + wp[c, 80:81, cols]
        js = slice(0, 8) if cy == 0 else slice(8, 17)
        for b in range(BLOCKS):
            sx[d, 0, b, js] = acc[b, 0, js].astype(BF16)
            sx[d, 1, b, js] = acc[b, LO, js].astype(BF16)
            sy[d, cy, b] = acc[b, :, 16 * cy].astype(BF16)
        copies = exchange(d, cy)
        for copy in copies:
            copy.start()
        return copies

    def apply(d, now, later, scale, keep, close):
        copies = cells(d, 0) + cells(d, 1)

        def inner(i, carry):
            for b in range(BLOCKS):
                m = im[i]
                fresh = scale * (acc[b, i] * (m * (1.0 / half_width)) + bt[i] * y[now, b, i]) - keep * y[later, b, i]
                y[later, b, i] = fresh
                uf[b, i] = fresh * m
            return carry

        lax.fori_loop(0, EX, inner, 0)

        def add(b, i, j, part):
            y[later, b, i, j] = y[later, b, i, j] + (scale * (1.0 / half_width)) * im[i, j] * part.astype(F32)

        def refresh(b, i, j):
            uf[b, i, j] = y[later, b, i, j] * im[i, j]

        def arrive():
            for copy in copies:
                copy.wait()
            for b in range(BLOCKS):
                add(b, 0, slice(0, 17), rx[d, 0, b])
                add(b, slice(0, EX), 0, ry[d, 0, b])
                add(b, 0, 0, rd[d, 0, b])
                add(b, LO, slice(0, 17), rx[d, 1, b])
                add(b, slice(0, EX), 16, ry[d, 1, b])
                add(b, 0, 16, rd[d, 1, b])
                add(b, LO, 0, rd[d, 2, b])
                add(b, LO, 16, rd[d, 3, b])
                refresh(b, 0, slice(0, 17))
                refresh(b, LO, slice(0, 17))
                refresh(b, slice(1, LO), 0)
                refresh(b, slice(1, LO), 16)

        def arrive_last():
            for copy in copies:
                copy.wait()
            for b in range(BLOCKS):
                add(b, 0, slice(0, 16), rx[d, 0, b, 0:16])
                add(b, slice(0, LO), 0, ry[d, 0, b, 0:LO])
                add(b, 0, 0, rd[d, 0, b])

        if close:
            arrive()
            return None
        return arrive_last

    def step(d, carry):
        scale = jnp.where(d == 0, 1.0, 2.0).astype(F32)
        keep = jnp.where(d == 0, 0.0, 1.0).astype(F32)
        apply(d, lax.rem(d, 2), lax.rem(d + 1, 2), scale, keep, True)
        return carry

    lax.fori_loop(0, DEGREE - 1, step, 0)
    final = DEGREE % 2
    y[1 - final, :, LO] = jnp.zeros((BLOCKS, EY, EZ, W), F32)
    y[final, :, LO] = jnp.zeros((BLOCKS, EY, EZ, W), F32)
    y[1 - final, :, 0:LO, 16] = jnp.zeros((BLOCKS, LO, EZ, W), F32)
    y[final, :, 0:LO, 16] = jnp.zeros((BLOCKS, LO, EZ, W), F32)
    arrive_last = apply(DEGREE - 1, 1 - final, final, 2.0, 1.0, False)

    load.wait()
    for copy in rhalo:
        copy.wait()
    nres = rs.shape[-1]
    right = jnp.concatenate([y[final, b, :, 16].reshape(EX * EZ, W).astype(BF16) for b in range(BLOCKS)], axis=1)
    mloc[...] = lax.dot_general(
        rs[:, 16].reshape(EX * EZ, nres), right, (((0,), (0,)), ((), ())), preferred_element_type=F32
    )

    def product(i, carry):
        cols = [y[final, b, i, 0:16].reshape(256, W).astype(BF16) for b in range(BLOCKS)]
        right = jnp.concatenate(cols, axis=1)
        left = rs[i, 0:16].reshape(256, nres)
        mloc[...] += lax.dot_general(left, right, (((0,), (0,)), ((), ())), preferred_element_type=F32)
        return carry

    lax.fori_loop(0, EX, product, 0)

    span = CORES * 16
    for g in range(ZH * NXC):
        m1s[g] = (mloc[pl.ds(pl.multiple_of(g * span + (CORES - 1 - core) * 16, 16), 16), :] * norm_scale).astype(BF16)
    copy = remote(m1s, m1r, s1.at[0], r1.at[0], partner[0])
    copy.start()
    copy.wait()

    def both(g):
        own = mloc[pl.ds(pl.multiple_of(g * span + core * 16, 16), 16), :] * norm_scale
        return own + m1r[g].astype(F32)

    for zv in range(ZH):
        for k in range(1, NXC):
            m2s[k - 1, zv] = both(zv * NXC + (xc + k) % NXC).astype(BF16)
    copies = [remote(m2s.at[k], m2r.at[k], s2.at[k], r2.at[k], row[k]) for k in range(NXC - 1)]
    for copy in copies:
        copy.start()
    arrive_last()
    writes = [
        pltpu.make_async_copy(y.at[final, b, pl.ds(0, LO), pl.ds(0, 16)], out.at[b], osem.at[b])
        for b in range(BLOCKS)
    ]
    for copy in writes:
        copy.start()
    for copy in copies:
        copy.wait()
    for zv in range(ZH):
        total = both(zv * NXC + xc)
        for k in range(NXC - 1):
            total = total + m2r[k, zv].astype(F32)
        for half in range(ZL):
            m3s[zv * ZL + half] = total[half * 8 : half * 8 + 8]
    copies = [
        remote(m3s.at[(zi + k + 1) % nz], m3r.at[k], s3.at[k], r3.at[k], column[k]) for k in range(nz - 1)
    ]
    for copy in copies:
        copy.start()
    for copy in copies:
        copy.wait()
    total = m3s[zi]
    for k in range(nz - 1):
        total = total + m3r[k]
    m4s[...] = total
    m4r[p] = total
    copies = [remote(m4s, m4r.at[p], s4.at[k], r4.at[k], group[k]) for k in range(ndx - 1)]
    for copy in copies:
        copy.start()
    for copy in copies:
        copy.wait()
    for half in range(ZL):
        total = m4r[half * NYC]
        for k in range(1, NYC):
            total = total + m4r[half * NYC + k]
        margin[half * 8 : half * 8 + 8, :] = total
    for copy in writes:
        copy.wait()


def body(vectors, resident, inv_mass, potential, cell_matrix, connectivity):
    total_nodes = inv_mass.size * lax.axis_size("dx") * lax.axis_size("dy")
    norm_scale = 1.0 / math.sqrt(total_nodes)
    nres = resident.shape[-1]
    ndx, ndy = ZL * NYC, ZH * NXC * CORES
    nz = ZL * ZH
    rows = 16 * ndy
    vmem = pl.BlockSpec(memory_space=pltpu.VMEM)
    hbm = pl.BlockSpec(memory_space=pl.ANY)
    dma = pltpu.SemaphoreType.DMA

    def k(*refs):
        kernel(norm_scale, *refs)

    state = (BLOCKS, EX, EY, EZ, W)
    return pl.pallas_call(
        k,
        out_shape=(
            jax.ShapeDtypeStruct((BLOCKS, LO, 16, EZ, W), F32),
            jax.ShapeDtypeStruct((16, BLOCKS * W), F32),
        ),
        in_specs=[vmem, hbm, vmem, vmem, vmem, vmem],
        out_specs=(hbm, vmem),
        scratch_shapes=[
            pltpu.VMEM((KP, KP), BF16),
            pltpu.VMEM((NCELL, KP, KP), BF16),
            pltpu.VMEM(state, F32),
            pltpu.VMEM(state, F32),
            pltpu.VMEM((2, *state), F32),
            pltpu.VMEM((EX, EY, EZ, W), F32),
            pltpu.VMEM((EX, EY, EZ, W), F32),
            pltpu.VMEM((NCELL, KP, BLOCKS * W), BF16),
            pltpu.VMEM((NCELL, KP - 648, BLOCKS * W), F32),
            pltpu.VMEM((rows, BLOCKS * W), F32),
            pltpu.VMEM((EX, EY, EZ, nres), BF16),
            pltpu.VMEM((NCELL, 1, KP), jnp.int32),
            pltpu.VMEM((2, EZ, LO * 16), F32),
            pltpu.VMEM((BLOCKS, 16, EZ, W), BF16),
            pltpu.VMEM((BLOCKS, LO, EZ, W), BF16),
            pltpu.VMEM((BLOCKS, EZ, W), BF16),
            pltpu.VMEM((2, EZ, LO * 16), F32),
            pltpu.VMEM((2, EZ, LO * 16), F32),
            pltpu.VMEM((2, EZ, LO * 16), F32),
            pltpu.VMEM((DEGREE, 2, BLOCKS, EY, EZ, W), BF16),
            pltpu.VMEM((DEGREE, 2, BLOCKS, EX, EZ, W), BF16),
            pltpu.VMEM((DEGREE, 2, BLOCKS, EY, EZ, W), BF16),
            pltpu.VMEM((DEGREE, 2, BLOCKS, EX, EZ, W), BF16),
            pltpu.VMEM((DEGREE, 4, BLOCKS, EZ, W), BF16),
            pltpu.VMEM((ZH * NXC, 16, BLOCKS * W), BF16),
            pltpu.VMEM((ZH * NXC, 16, BLOCKS * W), BF16),
            pltpu.VMEM((NXC - 1, ZH, 16, BLOCKS * W), BF16),
            pltpu.VMEM((NXC - 1, ZH, 16, BLOCKS * W), BF16),
            pltpu.VMEM((nz, 8, BLOCKS * W), F32),
            pltpu.VMEM((nz - 1, 8, BLOCKS * W), F32),
            pltpu.VMEM((8, BLOCKS * W), F32),
            pltpu.VMEM((ndx, 8, BLOCKS * W), F32),
            dma((9,)), dma((9,)), dma((DEGREE, 10)), dma((DEGREE, 10)),
            dma((1,)), dma((1,)), dma((NXC - 1,)), dma((NXC - 1,)),
            dma((nz - 1,)), dma((nz - 1,)), dma((ndx - 1,)), dma((ndx - 1,)), dma((BLOCKS,)), dma((1,)),
        ],
        compiler_params=pltpu.CompilerParams(
            collective_id=0, has_side_effects=True, vmem_limit_bytes=44 * 1024 * 1024
        ),
    )(vectors, resident, inv_mass, potential, cell_matrix, connectivity)


def solution(mesh):
    return jax.shard_map(
        body,
        mesh=mesh,
        in_specs=(
            P(None, "dx", "dy", None, None),
            P("dx", "dy", None, None),
            P("dx", "dy", None),
            P("dx", "dy", None),
            P(),
            P("dx", "dy", None, None),
        ),
        out_specs=(P(None, "dx", "dy", None, None), P("dy", None)),
        check_vma=False,
    )
```

```python
import math

import jax
import jax.numpy as jnp
from jax import lax
from jax.experimental import pallas as pl
from jax.experimental.pallas import tpu as pltpu
from jax.sharding import PartitionSpec as P

MESH = pl.DeviceIdType.MESH
BLOCKS = 2
DEGREE = 3
NCELL = 4
KP = 768
LO, EX, EY, EZ = 8, 9, 17, 16
W = 128
center_shift = 1.2
half_width = 2.0
ZL, NYC = 2, 4
ZH, NXC, CORES = 4, 4, 2
F32, BF16 = jnp.float32, jnp.bfloat16


def kernel(
    norm_scale, vec_in, res, mass_in, pot_in, amat_in, conn_in, out, margin,
    vec, mass, pot, amat, conn,
    ap, ac, acc, uf, y, im, bt, ub, wp, mloc, rs, posr, ct,
    xh, yh, dh, cx, cy_, cd, sx, sy, rx, ry, rd,
    m1s, m1r, m2s, m2r, m3s, m3r, m4s, m4r,
    hs_sem, hr_sem, es_sem, er_sem, s1, r1, s2, r2, s3, r3, s4, r4, osem, lsem,
):
    p = lax.axis_index("dx")
    q = lax.axis_index("dy")
    ndx, ndy = ZL * NYC, ZH * NXC * CORES
    zl, yc = p // NYC, p % NYC
    core, xc, zh = q % CORES, (q // CORES) % NXC, q // (CORES * NXC)
    pm, pp = (p + ndx - 1) % ndx, (p + 1) % ndx
    qm, qp = (q + ndy - 1) % ndy, (q + 1) % ndy

    def dy_of(zhv, xv, cv):
        return (zhv * NXC + xv) * CORES + cv

    neighbours = [(pm, q), (pp, q), (p, qm), (p, qp), (pm, qm), (pp, qp), (pm, qp), (pp, qm)]
    partner = [(p, dy_of(zh, xc, CORES - 1 - core))]
    row = [(p, dy_of(zh, (xc + k) % NXC, core)) for k in range(1, NXC)]
    nz = ZL * ZH
    zi = zh * ZL + zl
    column = []
    for k in range(1, nz):
        other = (zi + k) % nz
        column.append(((other % ZL) * NYC + yc, dy_of(other // ZL, xc, core)))
    group = [((p + k) % ndx, q) for k in range(1, ndx)]

    barrier = pltpu.get_barrier_semaphore()
    greeted = neighbours + partner + row + column + group
    for device in greeted:
        pl.semaphore_signal(barrier, inc=1, device_id=device, device_id_type=MESH)
    loads = [
        pltpu.make_async_copy(src, dst, lsem.at[n + 1])
        for n, (src, dst) in enumerate(
            [(mass_in, mass), (pot_in, pot), (conn_in, conn), (amat_in, amat), (vec_in, vec)]
        )
    ]
    for copy in loads:
        copy.start()
    load = pltpu.make_async_copy(res, rs.at[pl.ds(0, LO), pl.ds(0, 16)], lsem.at[0])
    load.start()

    def remote(src, dst, ssem, rsem, device):
        return pltpu.make_async_remote_copy(
            src_ref=src, dst_ref=dst, send_sem=ssem, recv_sem=rsem, device_id=device, device_id_type=MESH
        )

    for copy in loads:
        copy.wait()
    ct[0] = mass[...].reshape(LO * 16, EZ).T
    ct[1] = pot[...].reshape(LO * 16, EZ).T

    index = conn[0, 0]
    cell = lax.broadcasted_iota(jnp.int32, index.shape, 0)
    k = index & 15
    t = index >> 4
    i = (t * 241) >> 12
    j = t - i * EY - 8 * (cell >> 1)
    inside = (k >> 3) == (cell & 1)
    plane = jnp.where(j < 8, 648 + i * 8 + j, 720 + i)
    where = jnp.where(inside, (i * 9 + j) * 8 + (k & 7), plane)
    posr[...] = jnp.full(posr.shape, -1, jnp.int32)
    nc = index.shape[1]
    for c in range(NCELL):
        posr[c, :, 0:nc] = where[c : c + 1]
    ap[...] = jnp.zeros_like(ap)
    ap[0:nc, 0:nc] = amat[...]

    def spread(tile, lane):
        return jnp.broadcast_to(tile[:, lane : lane + 1], (EZ, W))

    def coefs(i, j, mass_ij, pot_ij):
        im[i, j] = mass_ij
        bt[i, j] = (pot_ij - center_shift) * (1.0 / half_width)

    for i in range(LO):
        for j in range(16):
            coefs(i, j, spread(ct[0], i * 16 + j), spread(ct[1], i * 16 + j))

    def permute(c, carry):
        onehot = (lax.broadcasted_iota(jnp.int32, (KP, KP), 0) == posr[c]).astype(F32).astype(BF16)
        rows = jnp.dot(onehot, ap[...], preferred_element_type=F32).astype(BF16)
        ac[c] = lax.dot_general(rows, onehot, (((1,), (1,)), ((), ())), preferred_element_type=F32).astype(BF16)
        return carry

    lax.fori_loop(0, 1, permute, 0)

    pl.semaphore_wait(barrier, len(greeted))
    halo = [
        remote(ct, cd, hs_sem.at[5], hr_sem.at[5], (pm, qm)),
        remote(vec.at[:, 0, 0], dh, hs_sem.at[2], hr_sem.at[2], (pm, qm)),
        remote(ct, cx, hs_sem.at[3], hr_sem.at[3], (pm, q)),
        remote(ct, cy_, hs_sem.at[4], hr_sem.at[4], (p, qm)),
        remote(vec.at[:, 0], xh, hs_sem.at[0], hr_sem.at[0], (pm, q)),
        remote(vec.at[:, :, 0], yh, hs_sem.at[1], hr_sem.at[1], (p, qm)),
    ]
    for copy in halo:
        copy.start()
    rhalo = [
        remote(res.at[:, 0], rs.at[pl.ds(0, LO), 16], hs_sem.at[7], hr_sem.at[7], (p, qm)),
        remote(res.at[0, pl.ds(0, 8)], rs.at[LO, pl.ds(0, 8)], hs_sem.at[6], hr_sem.at[6], (pm, q)),
        remote(res.at[0, 0], rs.at[LO, 16], hs_sem.at[8], hr_sem.at[8], (pm, qm)),
        remote(res.at[0, pl.ds(8, 8)], rs.at[LO, pl.ds(8, 8)], hs_sem.at[9], hr_sem.at[9], (pm, q)),
    ]
    for copy in rhalo[:2]:
        copy.start()

    def fill(i, carry):
        for b in range(BLOCKS):
            value = vec[b, i].astype(F32)
            y[0, b, i, 0:16] = value
            uf[b, i, 0:16] = value * im[i, 0:16]
        return carry

    lax.fori_loop(0, LO, fill, 0)
    lax.fori_loop(1, NCELL, permute, 0)

    for copy in halo:
        copy.wait()
    for j in range(16):
        coefs(LO, j, spread(cx[0], j), spread(cx[1], j))
    for i in range(LO):
        coefs(i, 16, spread(cy_[0], i * 16), spread(cy_[1], i * 16))
    coefs(LO, 16, spread(cd[0], 0), spread(cd[1], 0))
    for b in range(BLOCKS):
        value = xh[b].astype(F32)
        y[0, b, LO, 0:16] = value
        uf[b, LO, 0:16] = value * im[LO, 0:16]
        value = yh[b].astype(F32)
        y[0, b, 0:LO, 16] = value
        uf[b, 0:LO, 16] = value * im[0:LO, 16]
        value = dh[b].astype(F32)
        y[0, b, LO, 16] = value
        uf[b, LO, 16] = value * im[LO, 16]

    def exchange(d, b):
        plan = [
            (sx.at[d, 1, b, 16], rd.at[d, 0, b], (pp, qp)),
            (sx.at[d, 0, b, 0], rd.at[d, 3, b], (pm, qm)),
            (sx.at[d, 0, b, 16], rd.at[d, 2, b], (pm, qp)),
            (sx.at[d, 1, b, 0], rd.at[d, 1, b], (pp, qm)),
            (sy.at[d, 1, b], ry.at[d, 0, b], (p, qp)),
            (sy.at[d, 0, b], ry.at[d, 1, b], (p, qm)),
            (sx.at[d, 1, b], rx.at[d, 0, b], (pp, q)),
            (sx.at[d, 0, b], rx.at[d, 1, b], (pm, q)),
        ]
        wanted = (0, 4, 6) if d == DEGREE - 1 else range(8)
        return [
            remote(s, t, es_sem.at[d, b, n], er_sem.at[d, b, n], to)
            for n, (s, t, to) in enumerate(plan)
            if n in wanted
        ]

    def cells(d, b):
        flat = uf.at[b].reshape(EX * EY * EZ, W)
        total = acc.at[b].reshape(EX * EY * EZ, W)
        for cy in range(2):
            for cz in range(2):
                c = cy * 2 + cz
                kp = (8 * cz + 8) % 16
                ks = slice(8 * cz, 8 * cz + 8)
                main = uf[b, :, 8 * cy : 8 * cy + 9, ks, :].reshape(648, W)
                planes = [flat[pl.ds((i * EY + 8 * cy) * EZ + kp, 8, EZ), :] for i in range(EX)]
                start = (8 * cy + 8) * EZ + kp
                line = flat[pl.ds(start, 8, EY * EZ), :]
                last = flat[pl.ds(start + 8 * EY * EZ, 1), :]
                first = lax.broadcasted_iota(jnp.int32, (8, W), 0) == 0
                last = jnp.where(first, jnp.broadcast_to(last, (8, W)), 0.0)
                whole = jnp.concatenate([main] + planes + [line, last, jnp.zeros((32, W), F32)], axis=0)
                ub[b, c] = whole.astype(BF16)
                w = jnp.dot(ac[c], ub[b, c], preferred_element_type=F32)
                wp[b, c] = w[648:]
                block = w[:648].reshape(EX, 9, 8, W)
                if cy == 0:
                    acc[b, :, 0:9, ks, :] = block
                else:
                    acc[b, :, 8, ks, :] += block[:, 0]
                    acc[b, :, 9:17, ks, :] = block[:, 1:]
            for cz in range(2):
                c = cy * 2 + cz
                kp = (8 * cz + 8) % 16
                for i in range(EX):
                    where = pl.ds((i * EY + 8 * cy) * EZ + kp, 8, EZ)
                    total[where, :] = total[where, :] + wp[b, c, 8 * i : 8 * i + 8]
                start = (8 * cy + 8) * EZ + kp
                where = pl.ds(start, 8, EY * EZ)
                total[where, :] = total[where, :] + wp[b, c, 72:80]
                where = pl.ds(start + 8 * EY * EZ, 1)
                total[where, :] = total[where, :] + wp[b, c, 80:81]
        sx[d, 0, b] = acc[b, 0].astype(BF16)
        sx[d, 1, b] = acc[b, LO].astype(BF16)
        sy[d, 0, b] = acc[b, :, 0].astype(BF16)
        sy[d, 1, b] = acc[b, :, 16].astype(BF16)
        for copy in exchange(d, b):
            copy.start()

    def update(d, b):
        now, later = d % 2, (d + 1) % 2

        def inner(i, carry):
            m = im[i]
            fresh = acc[b, i] * (m * (1.0 / half_width)) + bt[i] * y[now, b, i]
            if d > 0:
                fresh = 2.0 * fresh - y[later, b, i]
            y[later, b, i] = fresh
            if d < DEGREE - 1:
                uf[b, i] = fresh * m
            return carry

        lax.fori_loop(0, EX, inner, 0)

    def arrive(d, b):
        later = (d + 1) % 2
        factor = (1.0 if d == 0 else 2.0) / half_width

        def add(i, j, part):
            y[later, b, i, j] = y[later, b, i, j] + factor * im[i, j] * part.astype(F32)

        def refresh(i, j):
            uf[b, i, j] = y[later, b, i, j] * im[i, j]

        for copy in exchange(d, b):
            copy.wait()
        if d == DEGREE - 1:
            add(0, slice(0, 16), rx[d, 0, b, 0:16])
            add(slice(0, LO), 0, ry[d, 0, b, 0:LO])
            add(0, 0, rd[d, 0, b])
            return
        add(0, slice(0, 17), rx[d, 0, b])
        add(slice(0, EX), 0, ry[d, 0, b])
        add(0, 0, rd[d, 0, b])
        add(LO, slice(0, 17), rx[d, 1, b])
        add(slice(0, EX), 16, ry[d, 1, b])
        add(0, 16, rd[d, 1, b])
        add(LO, 0, rd[d, 2, b])
        add(LO, 16, rd[d, 3, b])
        refresh(0, slice(0, 17))
        refresh(LO, slice(0, 17))
        refresh(slice(1, LO), 0)
        refresh(slice(1, LO), 16)

    for d in range(DEGREE):
        for b in range(BLOCKS):
            if d > 0:
                arrive(d - 1, b)
            if d == DEGREE - 1:
                for side in range(2):
                    y[side, b, LO] = jnp.zeros((EY, EZ, W), F32)
                    y[side, b, 0:LO, 16] = jnp.zeros((LO, EZ, W), F32)
            cells(d, b)
            if d == 0 and b == BLOCKS - 1:
                for copy in rhalo[2:]:
                    copy.start()
            update(d, b)
    final = DEGREE % 2

    load.wait()
    for copy in rhalo:
        copy.wait()
    nres = rs.shape[-1]
    right = jnp.concatenate([y[final, b, :, 16].reshape(EX * EZ, W).astype(BF16) for b in range(BLOCKS)], axis=1)
    mloc[...] = lax.dot_general(
        rs[:, 16].reshape(EX * EZ, nres), right, (((0,), (0,)), ((), ())), preferred_element_type=F32
    )

    def product(i, carry):
        cols = [y[final, b, i, 0:16].reshape(256, W).astype(BF16) for b in range(BLOCKS)]
        right = jnp.concatenate(cols, axis=1)
        left = rs[i, 0:16].reshape(256, nres)
        mloc[...] += lax.dot_general(left, right, (((0,), (0,)), ((), ())), preferred_element_type=F32)
        return carry

    lax.fori_loop(0, EX, product, 0)

    span = CORES * 16
    for g in range(ZH * NXC):
        m1s[g] = (mloc[pl.ds(pl.multiple_of(g * span + (CORES - 1 - core) * 16, 16), 16), :] * norm_scale).astype(BF16)
    copy = remote(m1s, m1r, s1.at[0], r1.at[0], partner[0])
    copy.start()
    copy.wait()

    def both(g):
        own = mloc[pl.ds(pl.multiple_of(g * span + core * 16, 16), 16), :] * norm_scale
        return own + m1r[g].astype(F32)

    for zv in range(ZH):
        for k in range(1, NXC):
            m2s[k - 1, zv] = both(zv * NXC + (xc + k) % NXC).astype(BF16)
    copies = [remote(m2s.at[k], m2r.at[k], s2.at[k], r2.at[k], row[k]) for k in range(NXC - 1)]
    for copy in copies:
        copy.start()
    for b in range(BLOCKS):
        arrive(DEGREE - 1, b)
    writes = [
        pltpu.make_async_copy(y.at[final, b, pl.ds(0, LO), pl.ds(0, 16)], out.at[b], osem.at[b])
        for b in range(BLOCKS)
    ]
    for copy in writes:
        copy.start()
    for copy in copies:
        copy.wait()
    for zv in range(ZH):
        total = both(zv * NXC + xc)
        for k in range(NXC - 1):
            total = total + m2r[k, zv].astype(F32)
        for half in range(ZL):
            m3s[zv * ZL + half] = total[half * 8 : half * 8 + 8]
    copies = [
        remote(m3s.at[(zi + k + 1) % nz], m3r.at[k], s3.at[k], r3.at[k], column[k]) for k in range(nz - 1)
    ]
    for copy in copies:
        copy.start()
    for copy in copies:
        copy.wait()
    total = m3s[zi]
    for k in range(nz - 1):
        total = total + m3r[k]
    m4s[...] = total
    m4r[p] = total
    copies = [remote(m4s, m4r.at[p], s4.at[k], r4.at[k], group[k]) for k in range(ndx - 1)]
    for copy in copies:
        copy.start()
    for copy in copies:
        copy.wait()
    for half in range(ZL):
        total = m4r[half * NYC]
        for k in range(1, NYC):
            total = total + m4r[half * NYC + k]
        margin[half * 8 : half * 8 + 8, :] = total
    for copy in writes:
        copy.wait()


def body(vectors, resident, inv_mass, potential, cell_matrix, connectivity):
    total_nodes = inv_mass.size * lax.axis_size("dx") * lax.axis_size("dy")
    norm_scale = 1.0 / math.sqrt(total_nodes)
    nres = resident.shape[-1]
    ndx, ndy = ZL * NYC, ZH * NXC * CORES
    nz = ZL * ZH
    rows = 16 * ndy
    vmem = pl.BlockSpec(memory_space=pltpu.VMEM)
    dma = pltpu.SemaphoreType.DMA

    def k(*refs):
        kernel(norm_scale, *refs)

    state = (BLOCKS, EX, EY, EZ, W)
    return pl.pallas_call(
        k,
        out_shape=(
            jax.ShapeDtypeStruct((BLOCKS, LO, 16, EZ, W), F32),
            jax.ShapeDtypeStruct((16, BLOCKS * W), F32),
        ),
        in_specs=[pl.BlockSpec(memory_space=pltpu.HBM)] * 6,
        out_specs=(pl.BlockSpec(memory_space=pl.ANY), vmem),
        scratch_shapes=[
            pltpu.VMEM(vectors.shape, BF16),
            pltpu.VMEM(inv_mass.shape, F32),
            pltpu.VMEM(potential.shape, F32),
            pltpu.VMEM(cell_matrix.shape, BF16),
            pltpu.VMEM(connectivity.shape, jnp.int32),
            pltpu.VMEM((KP, KP), BF16),
            pltpu.VMEM((NCELL, KP, KP), BF16),
            pltpu.VMEM(state, F32),
            pltpu.VMEM(state, F32),
            pltpu.VMEM((2, *state), F32),
            pltpu.VMEM((EX, EY, EZ, W), F32),
            pltpu.VMEM((EX, EY, EZ, W), F32),
            pltpu.VMEM((BLOCKS, NCELL, KP, W), BF16),
            pltpu.VMEM((BLOCKS, NCELL, KP - 648, W), F32),
            pltpu.VMEM((rows, BLOCKS * W), F32),
            pltpu.VMEM((EX, EY, EZ, nres), BF16),
            pltpu.VMEM((NCELL, 1, KP), jnp.int32),
            pltpu.VMEM((2, EZ, LO * 16), F32),
            pltpu.VMEM((BLOCKS, 16, EZ, W), BF16),
            pltpu.VMEM((BLOCKS, LO, EZ, W), BF16),
            pltpu.VMEM((BLOCKS, EZ, W), BF16),
            pltpu.VMEM((2, EZ, LO * 16), F32),
            pltpu.VMEM((2, EZ, LO * 16), F32),
            pltpu.VMEM((2, EZ, LO * 16), F32),
            pltpu.VMEM((DEGREE, 2, BLOCKS, EY, EZ, W), BF16),
            pltpu.VMEM((DEGREE, 2, BLOCKS, EX, EZ, W), BF16),
            pltpu.VMEM((DEGREE, 2, BLOCKS, EY, EZ, W), BF16),
            pltpu.VMEM((DEGREE, 2, BLOCKS, EX, EZ, W), BF16),
            pltpu.VMEM((DEGREE, 4, BLOCKS, EZ, W), BF16),
            pltpu.VMEM((ZH * NXC, 16, BLOCKS * W), BF16),
            pltpu.VMEM((ZH * NXC, 16, BLOCKS * W), BF16),
            pltpu.VMEM((NXC - 1, ZH, 16, BLOCKS * W), BF16),
            pltpu.VMEM((NXC - 1, ZH, 16, BLOCKS * W), BF16),
            pltpu.VMEM((nz, 8, BLOCKS * W), F32),
            pltpu.VMEM((nz - 1, 8, BLOCKS * W), F32),
            pltpu.VMEM((8, BLOCKS * W), F32),
            pltpu.VMEM((ndx, 8, BLOCKS * W), F32),
            dma((10,)), dma((10,)), dma((DEGREE, BLOCKS, 8)), dma((DEGREE, BLOCKS, 8)),
            dma((1,)), dma((1,)), dma((NXC - 1,)), dma((NXC - 1,)),
            dma((nz - 1,)), dma((nz - 1,)), dma((ndx - 1,)), dma((ndx - 1,)), dma((BLOCKS,)), dma((6,)),
        ],
        compiler_params=pltpu.CompilerParams(
            collective_id=0, has_side_effects=True, vmem_limit_bytes=62914560
        ),
    )(vectors, resident, inv_mass, potential, cell_matrix, connectivity)


def solution(mesh):
    return jax.shard_map(
        body,
        mesh=mesh,
        in_specs=(
            P(None, "dx", "dy", None, None),
            P("dx", "dy", None, None),
            P("dx", "dy", None),
            P("dx", "dy", None),
            P(),
            P("dx", "dy", None, None),
        ),
        out_specs=(P(None, "dx", "dy", None, None), P("dy", None)),
        check_vma=False,
    )
```

```python
import math

import jax
import jax.numpy as jnp
from jax import lax
from jax.experimental import pallas as pl
from jax.experimental.pallas import tpu as pltpu
from jax.sharding import PartitionSpec as P

MESH = pl.DeviceIdType.MESH
BLOCKS = 2
DEGREE = 3
NCELL = 4
KP = 768
LO, EX, EY, EZ = 8, 9, 17, 16
W = 128
center_shift = 1.2
half_width = 2.0
ZL, NYC = 2, 4
ZH, NXC, CORES = 4, 4, 2
F32, BF16 = jnp.float32, jnp.bfloat16


def kernel(
    norm_scale, vec_in, res, mass_in, pot_in, amat_in, conn_in, out, margin,
    vec, mass, pot, amat, conn,
    ap, ac, acc, uf, y, im, bt, ub, wp, mloc, rs, rt, vb, posr, ct,
    xh, yh, dh, cx, cy_, cd, sx, sy, rx, ry, rd,
    m1s, m1r, m2s, m2r, m3s, m3r, m4s, m4r,
    hs_sem, hr_sem, es_sem, er_sem, s1, r1, s2, r2, s3, r3, s4, r4, osem, lsem,
):
    p = lax.axis_index("dx")
    q = lax.axis_index("dy")
    ndx, ndy = ZL * NYC, ZH * NXC * CORES
    zl, yc = p // NYC, p % NYC
    core, xc, zh = q % CORES, (q // CORES) % NXC, q // (CORES * NXC)
    pm, pp = (p + ndx - 1) % ndx, (p + 1) % ndx
    qm, qp = (q + ndy - 1) % ndy, (q + 1) % ndy

    def dy_of(zhv, xv, cv):
        return (zhv * NXC + xv) * CORES + cv

    neighbours = [(pm, q), (pp, q), (p, qm), (p, qp), (pm, qm), (pp, qp), (pm, qp), (pp, qm)]
    partner = [(p, dy_of(zh, xc, CORES - 1 - core))]
    row = [(p, dy_of(zh, (xc + k) % NXC, core)) for k in range(1, NXC)]
    nz = ZL * ZH
    zi = zh * ZL + zl
    column = []
    for k in range(1, nz):
        other = (zi + k) % nz
        column.append(((other % ZL) * NYC + yc, dy_of(other // ZL, xc, core)))
    group = [((p + k) % ndx, q) for k in range(1, ndx)]

    barrier = pltpu.get_barrier_semaphore()
    greeted = neighbours + partner + row + column + group
    for device in greeted:
        pl.semaphore_signal(barrier, inc=1, device_id=device, device_id_type=MESH)
    loads = [
        pltpu.make_async_copy(src, dst, lsem.at[n + 1])
        for n, (src, dst) in enumerate(
            [(mass_in, mass), (pot_in, pot), (conn_in, conn), (amat_in, amat), (vec_in, vec)]
        )
    ]
    for copy in loads:
        copy.start()
    load = pltpu.make_async_copy(res, rs.at[pl.ds(0, LO), pl.ds(0, 16)], lsem.at[0])
    load.start()

    def remote(src, dst, ssem, rsem, device):
        return pltpu.make_async_remote_copy(
            src_ref=src, dst_ref=dst, send_sem=ssem, recv_sem=rsem, device_id=device, device_id_type=MESH
        )

    for copy in loads:
        copy.wait()
    ct[0] = mass[...].reshape(LO * 16, EZ).T
    ct[1] = pot[...].reshape(LO * 16, EZ).T

    index = conn[0, 0]
    cell = lax.broadcasted_iota(jnp.int32, index.shape, 0)
    k = index & 15
    t = index >> 4
    i = (t * 241) >> 12
    j = t - i * EY - 8 * (cell >> 1)
    inside = (k >> 3) == (cell & 1)
    plane = jnp.where(j < 8, 648 + i * 8 + j, 720 + i)
    where = jnp.where(inside, (i * 9 + j) * 8 + (k & 7), plane)
    posr[...] = jnp.full(posr.shape, -1, jnp.int32)
    nc = index.shape[1]
    for c in range(NCELL):
        posr[c, :, 0:nc] = where[c : c + 1]
    ap[...] = jnp.zeros_like(ap)
    ap[0:nc, 0:nc] = amat[...]

    def spread(tile, lane):
        return jnp.broadcast_to(tile[:, lane : lane + 1], (EZ, W))

    def coefs(i, j, mass_ij, pot_ij):
        im[i, j] = mass_ij
        bt[i, j] = (pot_ij - center_shift) * (1.0 / half_width)

    for i in range(LO):
        for j in range(16):
            coefs(i, j, spread(ct[0], i * 16 + j), spread(ct[1], i * 16 + j))

    def permute(c, carry):
        onehot = (lax.broadcasted_iota(jnp.int32, (KP, KP), 0) == posr[c]).astype(F32).astype(BF16)
        rows = jnp.dot(onehot, ap[...], preferred_element_type=F32).astype(BF16)
        ac[c] = lax.dot_general(rows, onehot, (((1,), (1,)), ((), ())), preferred_element_type=F32).astype(BF16)
        return carry

    lax.fori_loop(0, 1, permute, 0)

    pl.semaphore_wait(barrier, len(greeted))
    halo = [
        remote(ct, cd, hs_sem.at[5], hr_sem.at[5], (pm, qm)),
        remote(vec.at[:, 0, 0], dh, hs_sem.at[2], hr_sem.at[2], (pm, qm)),
        remote(ct, cx, hs_sem.at[3], hr_sem.at[3], (pm, q)),
        remote(ct, cy_, hs_sem.at[4], hr_sem.at[4], (p, qm)),
        remote(vec.at[:, 0], xh, hs_sem.at[0], hr_sem.at[0], (pm, q)),
        remote(vec.at[:, :, 0], yh, hs_sem.at[1], hr_sem.at[1], (p, qm)),
    ]
    for copy in halo:
        copy.start()
    rhalo = [
        remote(res.at[:, 0], rs.at[pl.ds(0, LO), 16], hs_sem.at[7], hr_sem.at[7], (p, qm)),
        remote(res.at[0, pl.ds(0, 8)], rs.at[LO, pl.ds(0, 8)], hs_sem.at[6], hr_sem.at[6], (pm, q)),
        remote(res.at[0, 0], rs.at[LO, 16], hs_sem.at[8], hr_sem.at[8], (pm, qm)),
        remote(res.at[0, pl.ds(8, 8)], rs.at[LO, pl.ds(8, 8)], hs_sem.at[9], hr_sem.at[9], (pm, q)),
    ]
    for copy in rhalo[:2]:
        copy.start()

    def fill(i, carry):
        for b in range(BLOCKS):
            value = vec[b, i].astype(F32)
            y[0, b, i, 0:16] = value
            uf[b, i, 0:16] = value * im[i, 0:16]
        return carry

    lax.fori_loop(0, LO, fill, 0)
    tail = EX * 256
    rt[:, tail:] = jnp.zeros((rt.shape[0], 256), BF16)
    for b in range(BLOCKS):
        vb[b, tail:] = jnp.zeros((256, W), BF16)
    lax.fori_loop(1, NCELL, permute, 0)

    for copy in halo:
        copy.wait()
    for j in range(16):
        coefs(LO, j, spread(cx[0], j), spread(cx[1], j))
    for i in range(LO):
        coefs(i, 16, spread(cy_[0], i * 16), spread(cy_[1], i * 16))
    coefs(LO, 16, spread(cd[0], 0), spread(cd[1], 0))
    for b in range(BLOCKS):
        value = xh[b].astype(F32)
        y[0, b, LO, 0:16] = value
        uf[b, LO, 0:16] = value * im[LO, 0:16]
        value = yh[b].astype(F32)
        y[0, b, 0:LO, 16] = value
        uf[b, 0:LO, 16] = value * im[0:LO, 16]
        value = dh[b].astype(F32)
        y[0, b, LO, 16] = value
        uf[b, LO, 16] = value * im[LO, 16]

    def exchange(d, b):
        plan = [
            (sx.at[d, 1, b, 16], rd.at[d, 0, b], (pp, qp)),
            (sx.at[d, 0, b, 0], rd.at[d, 3, b], (pm, qm)),
            (sx.at[d, 0, b, 16], rd.at[d, 2, b], (pm, qp)),
            (sx.at[d, 1, b, 0], rd.at[d, 1, b], (pp, qm)),
            (sy.at[d, 1, b], ry.at[d, 0, b], (p, qp)),
            (sy.at[d, 0, b], ry.at[d, 1, b], (p, qm)),
            (sx.at[d, 1, b], rx.at[d, 0, b], (pp, q)),
            (sx.at[d, 0, b], rx.at[d, 1, b], (pm, q)),
        ]
        wanted = (0, 4, 6) if d == DEGREE - 1 else range(8)
        return [
            remote(s, t, es_sem.at[d, b, n], er_sem.at[d, b, n], to)
            for n, (s, t, to) in enumerate(plan)
            if n in wanted
        ]

    def cells(d, b):
        flat = uf.at[b].reshape(EX * EY * EZ, W)
        total = acc.at[b].reshape(EX * EY * EZ, W)
        for cy in range(2):
            for cz in range(2):
                c = cy * 2 + cz
                kp = (8 * cz + 8) % 16
                ks = slice(8 * cz, 8 * cz + 8)
                main = uf[b, :, 8 * cy : 8 * cy + 9, ks, :].reshape(648, W)
                planes = [flat[pl.ds((i * EY + 8 * cy) * EZ + kp, 8, EZ), :] for i in range(EX)]
                start = (8 * cy + 8) * EZ + kp
                line = flat[pl.ds(start, 8, EY * EZ), :]
                last = flat[pl.ds(start + 8 * EY * EZ, 1), :]
                first = lax.broadcasted_iota(jnp.int32, (8, W), 0) == 0
                last = jnp.where(first, jnp.broadcast_to(last, (8, W)), 0.0)
                whole = jnp.concatenate([main] + planes + [line, last, jnp.zeros((32, W), F32)], axis=0)
                ub[b, c] = whole.astype(BF16)
                w = jnp.dot(ac[c], ub[b, c], preferred_element_type=F32)
                wp[b, c] = w[648:]
                block = w[:648].reshape(EX, 9, 8, W)
                if cy == 0:
                    acc[b, :, 0:9, ks, :] = block
                else:
                    acc[b, :, 8, ks, :] += block[:, 0]
                    acc[b, :, 9:17, ks, :] = block[:, 1:]
            for cz in range(2):
                c = cy * 2 + cz
                kp = (8 * cz + 8) % 16
                for i in range(EX):
                    where = pl.ds((i * EY + 8 * cy) * EZ + kp, 8, EZ)
                    total[where, :] = total[where, :] + wp[b, c, 8 * i : 8 * i + 8]
                start = (8 * cy + 8) * EZ + kp
                where = pl.ds(start, 8, EY * EZ)
                total[where, :] = total[where, :] + wp[b, c, 72:80]
                where = pl.ds(start + 8 * EY * EZ, 1)
                total[where, :] = total[where, :] + wp[b, c, 80:81]
        sx[d, 0, b] = acc[b, 0].astype(BF16)
        sx[d, 1, b] = acc[b, LO].astype(BF16)
        sy[d, 0, b] = acc[b, :, 0].astype(BF16)
        sy[d, 1, b] = acc[b, :, 16].astype(BF16)
        for copy in exchange(d, b):
            copy.start()

    def update(d, b):
        now, later = d % 2, (d + 1) % 2

        def inner(i, carry):
            m = im[i]
            fresh = acc[b, i] * (m * (1.0 / half_width)) + bt[i] * y[now, b, i]
            if d > 0:
                fresh = 2.0 * fresh - y[later, b, i]
            y[later, b, i] = fresh
            if d < DEGREE - 1:
                uf[b, i] = fresh * m
            else:
                vb[b, pl.ds(pl.multiple_of(i * 256, 256), 256)] = fresh[0:16].reshape(256, W).astype(BF16)
                vb[b, pl.ds(pl.multiple_of(tail + i * EZ, EZ), EZ)] = fresh[16].astype(BF16)
            return carry

        lax.fori_loop(0, EX, inner, 0)

    def arrive(d, b):
        later = (d + 1) % 2
        factor = (1.0 if d == 0 else 2.0) / half_width

        def add(i, j, part):
            y[later, b, i, j] = y[later, b, i, j] + factor * im[i, j] * part.astype(F32)

        def refresh(i, j):
            uf[b, i, j] = y[later, b, i, j] * im[i, j]

        for copy in exchange(d, b):
            copy.wait()
        if d == DEGREE - 1:
            add(0, slice(0, 16), rx[d, 0, b, 0:16])
            add(slice(0, LO), 0, ry[d, 0, b, 0:LO])
            add(0, 0, rd[d, 0, b])
            return
        add(0, slice(0, 17), rx[d, 0, b])
        add(slice(0, EX), 0, ry[d, 0, b])
        add(0, 0, rd[d, 0, b])
        add(LO, slice(0, 17), rx[d, 1, b])
        add(slice(0, EX), 16, ry[d, 1, b])
        add(0, 16, rd[d, 1, b])
        add(LO, 0, rd[d, 2, b])
        add(LO, 16, rd[d, 3, b])
        refresh(0, slice(0, 17))
        refresh(LO, slice(0, 17))
        refresh(slice(1, LO), 0)
        refresh(slice(1, LO), 16)

    nres = rs.shape[-1]
    span = CORES * 16

    def turn_own():
        load.wait()
        for i in range(LO):
            rt[:, i * 256 : (i + 1) * 256] = rs[i, 0:16].reshape(256, nres).T

    def turn_halo():
        for copy in rhalo:
            copy.wait()
        rt[:, LO * 256 : EX * 256] = rs[LO, 0:16].reshape(256, nres).T
        rt[:, tail : tail + EX * EZ] = rs[:, 16].reshape(EX * EZ, nres).T

    def both(b, g):
        own = mloc[b, pl.ds(pl.multiple_of(g * span + core * 16, 16), 16), :]
        return own + m1r[b, g].astype(F32)

    def to_partner(b):
        return remote(m1s.at[b], m1r.at[b], s1.at[b], r1.at[b], partner[0])

    def to_row(b):
        return [remote(m2s.at[b, k], m2r.at[b, k], s2.at[b, k], r2.at[b, k], row[k]) for k in range(NXC - 1)]

    def first(b):
        mloc[b] = jnp.dot(rt[...], vb[b], preferred_element_type=F32) * norm_scale
        for g in range(ZH * NXC):
            where = pl.ds(pl.multiple_of(g * span + (CORES - 1 - core) * 16, 16), 16)
            m1s[b, g] = mloc[b, where, :].astype(BF16)
        to_partner(b).start()

    def second(b):
        to_partner(b).wait()
        for zv in range(ZH):
            for k in range(1, NXC):
                m2s[b, k - 1, zv] = both(b, zv * NXC + (xc + k) % NXC).astype(BF16)
        for copy in to_row(b):
            copy.start()

    for d in range(DEGREE):
        for b in range(BLOCKS):
            if d > 0:
                arrive(d - 1, b)
            if d == DEGREE - 1:
                for side in range(2):
                    y[side, b, LO] = jnp.zeros((EY, EZ, W), F32)
                    y[side, b, 0:LO, 16] = jnp.zeros((LO, EZ, W), F32)
            cells(d, b)
            if d == 0 and b == BLOCKS - 1:
                for copy in rhalo[2:]:
                    copy.start()
            if d == DEGREE - 1 and b > 0:
                second(b - 1)
            update(d, b)
            if d == DEGREE - 1:
                first(b)
        if d == 0:
            turn_own()
        if d == 1:
            turn_halo()
    second(BLOCKS - 1)
    final = DEGREE % 2
    for b in range(BLOCKS):
        arrive(DEGREE - 1, b)
    writes = [
        pltpu.make_async_copy(y.at[final, b, pl.ds(0, LO), pl.ds(0, 16)], out.at[b], osem.at[b])
        for b in range(BLOCKS)
    ]
    for copy in writes:
        copy.start()
    for b in range(BLOCKS):
        for copy in to_row(b):
            copy.wait()
        for zv in range(ZH):
            total = both(b, zv * NXC + xc)
            for k in range(NXC - 1):
                total = total + m2r[b, k, zv].astype(F32)
            for half in range(ZL):
                m3s[zv * ZL + half, :, b * W : (b + 1) * W] = total[half * 8 : half * 8 + 8]
    copies = [
        remote(m3s.at[(zi + k + 1) % nz], m3r.at[k], s3.at[k], r3.at[k], column[k]) for k in range(nz - 1)
    ]
    for copy in copies:
        copy.start()
    for copy in copies:
        copy.wait()
    total = m3s[zi]
    for k in range(nz - 1):
        total = total + m3r[k]
    m4s[...] = total
    m4r[p] = total
    copies = [remote(m4s, m4r.at[p], s4.at[k], r4.at[k], group[k]) for k in range(ndx - 1)]
    for copy in copies:
        copy.start()
    for copy in copies:
        copy.wait()
    for half in range(ZL):
        total = m4r[half * NYC]
        for k in range(1, NYC):
            total = total + m4r[half * NYC + k]
        margin[half * 8 : half * 8 + 8, :] = total
    for copy in writes:
        copy.wait()


def body(vectors, resident, inv_mass, potential, cell_matrix, connectivity):
    total_nodes = inv_mass.size * lax.axis_size("dx") * lax.axis_size("dy")
    norm_scale = 1.0 / math.sqrt(total_nodes)
    nres = resident.shape[-1]
    ndx, ndy = ZL * NYC, ZH * NXC * CORES
    nz = ZL * ZH
    rows = 16 * ndy
    vmem = pl.BlockSpec(memory_space=pltpu.VMEM)
    dma = pltpu.SemaphoreType.DMA

    def k(*refs):
        kernel(norm_scale, *refs)

    state = (BLOCKS, EX, EY, EZ, W)
    results = pl.pallas_call(
        k,
        out_shape=(
            jax.ShapeDtypeStruct((BLOCKS, LO, 16, EZ, W), F32),
            jax.ShapeDtypeStruct((16, BLOCKS * W), F32),
        ),
        in_specs=[pl.BlockSpec(memory_space=pltpu.HBM)] * 6,
        out_specs=(pl.BlockSpec(memory_space=pl.ANY), vmem),
        scratch_shapes=[
            pltpu.VMEM(vectors.shape, BF16),
            pltpu.VMEM(inv_mass.shape, F32),
            pltpu.VMEM(potential.shape, F32),
            pltpu.VMEM(cell_matrix.shape, BF16),
            pltpu.VMEM(connectivity.shape, jnp.int32),
            pltpu.VMEM((KP, KP), BF16),
            pltpu.VMEM((NCELL, KP, KP), BF16),
            pltpu.VMEM(state, F32),
            pltpu.VMEM(state, F32),
            pltpu.VMEM((2, *state), F32),
            pltpu.VMEM((EX, EY, EZ, W), F32),
            pltpu.VMEM((EX, EY, EZ, W), F32),
            pltpu.VMEM((BLOCKS, NCELL, KP, W), BF16),
            pltpu.VMEM((BLOCKS, NCELL, KP - 648, W), F32),
            pltpu.VMEM((BLOCKS, rows, W), F32),
            pltpu.VMEM((EX, EY, EZ, nres), BF16),
            pltpu.VMEM((nres, (EX + 1) * 256), BF16),
            pltpu.VMEM((BLOCKS, (EX + 1) * 256, W), BF16),
            pltpu.VMEM((NCELL, 1, KP), jnp.int32),
            pltpu.VMEM((2, EZ, LO * 16), F32),
            pltpu.VMEM((BLOCKS, 16, EZ, W), BF16),
            pltpu.VMEM((BLOCKS, LO, EZ, W), BF16),
            pltpu.VMEM((BLOCKS, EZ, W), BF16),
            pltpu.VMEM((2, EZ, LO * 16), F32),
            pltpu.VMEM((2, EZ, LO * 16), F32),
            pltpu.VMEM((2, EZ, LO * 16), F32),
            pltpu.VMEM((DEGREE, 2, BLOCKS, EY, EZ, W), BF16),
            pltpu.VMEM((DEGREE, 2, BLOCKS, EX, EZ, W), BF16),
            pltpu.VMEM((DEGREE, 2, BLOCKS, EY, EZ, W), BF16),
            pltpu.VMEM((DEGREE, 2, BLOCKS, EX, EZ, W), BF16),
            pltpu.VMEM((DEGREE, 4, BLOCKS, EZ, W), BF16),
            pltpu.VMEM((BLOCKS, ZH * NXC, 16, W), BF16),
            pltpu.VMEM((BLOCKS, ZH * NXC, 16, W), BF16),
            pltpu.VMEM((BLOCKS, NXC - 1, ZH, 16, W), BF16),
            pltpu.VMEM((BLOCKS, NXC - 1, ZH, 16, W), BF16),
            pltpu.VMEM((nz, 8, BLOCKS * W), F32),
            pltpu.VMEM((nz - 1, 8, BLOCKS * W), F32),
            pltpu.VMEM((8, BLOCKS * W), F32),
            pltpu.VMEM((ndx, 8, BLOCKS * W), F32),
            dma((10,)), dma((10,)), dma((DEGREE, BLOCKS, 8)), dma((DEGREE, BLOCKS, 8)),
            dma((BLOCKS,)), dma((BLOCKS,)), dma((BLOCKS, NXC - 1)), dma((BLOCKS, NXC - 1)),
            dma((nz - 1,)), dma((nz - 1,)), dma((ndx - 1,)), dma((ndx - 1,)), dma((BLOCKS,)), dma((6,)),
        ],
        compiler_params=pltpu.CompilerParams(
            collective_id=0, has_side_effects=True, vmem_limit_bytes=62914560
        ),
    )(vectors, resident, inv_mass, potential, cell_matrix, connectivity)
    in_hbm = pl.BlockSpec(memory_space=pltpu.HBM)
    return pl.pallas_call(
        hand_on,
        out_shape=tuple(jax.ShapeDtypeStruct(r.shape, F32) for r in results),
        in_specs=[in_hbm] * 2,
        out_specs=(in_hbm, in_hbm),
        scratch_shapes=[pltpu.VMEM(r.shape, F32) for r in results] + [dma((PIECES + 1,)), dma((PIECES + 1,))],
        compiler_params=pltpu.CompilerParams(vmem_limit_bytes=60 * 1024 * 1024),
    )(*results)


PIECES = 8


def hand_on(values, rows, values_out, rows_out, held, held_rows, isem, osem):
    plan = [(rows, held_rows, rows_out)]
    step = BLOCKS * LO // PIECES
    for n in range(PIECES):
        at = (n * step // LO, pl.ds(n * step % LO, step))
        plan.append((values.at[at], held.at[at], values_out.at[at]))
    copies = []
    for n, (src, mid, dst) in enumerate(plan):
        copies.append((pltpu.make_async_copy(src, mid, isem.at[n]), pltpu.make_async_copy(mid, dst, osem.at[n])))
    for into, _ in copies:
        into.start()
    for into, back in copies:
        into.wait()
        back.start()
    for _, back in copies:
        back.wait()


def solution(mesh):
    return jax.shard_map(
        body,
        mesh=mesh,
        in_specs=(
            P(None, "dx", "dy", None, None),
            P("dx", "dy", None, None),
            P("dx", "dy", None),
            P("dx", "dy", None),
            P(),
            P("dx", "dy", None, None),
        ),
        out_specs=(P(None, "dx", "dy", None, None), P("dy", None)),
        check_vma=False,
    )
```

```python
import math

import jax
import jax.numpy as jnp
from jax import lax
from jax.experimental import pallas as pl
from jax.experimental.pallas import tpu as pltpu
from jax.sharding import PartitionSpec as P

MESH = pl.DeviceIdType.MESH
BLOCKS = 2
DEGREE = 3
NCELL = 4
KP = 768
LO, EX, EY, EZ = 8, 9, 17, 16
W = 128
center_shift = 1.2
half_width = 2.0
ZL, NYC = 2, 4
ZH, NXC, CORES = 4, 4, 2
F32, BF16 = jnp.float32, jnp.bfloat16


def kernel(
    norm_scale, vec_in, res, mass_in, pot_in, amat_in, conn_in, out, margin,
    vec, mass, pot, amat, conn,
    ap, ac, acc, uf, y, im, bt, ub, wp, mloc, rs, rt, vb, posr, ct,
    xh, yh, dh, cx, cy_, cd, sx, sy, rx, ry, rd,
    m1s, m1r, m2s, m2r, m3f, m3s, m3r, m4s, m4r,
    hs_sem, hr_sem, es_sem, er_sem, s1, r1, s2, r2, s3, r3, s4, r4, osem, lsem,
):
    p = lax.axis_index("dx")
    q = lax.axis_index("dy")
    ndx, ndy = ZL * NYC, ZH * NXC * CORES
    zl, yc = p // NYC, p % NYC
    core, xc, zh = q % CORES, (q // CORES) % NXC, q // (CORES * NXC)
    pm, pp = (p + ndx - 1) % ndx, (p + 1) % ndx
    qm, qp = (q + ndy - 1) % ndy, (q + 1) % ndy

    def dy_of(zhv, xv, cv):
        return (zhv * NXC + xv) * CORES + cv

    neighbours = [(pm, q), (pp, q), (p, qm), (p, qp), (pm, qm), (pp, qp), (pm, qp), (pp, qm)]
    partner = [(p, dy_of(zh, xc, CORES - 1 - core))]
    row = [(p, dy_of(zh, (xc + k) % NXC, core)) for k in range(1, NXC)]
    nz = ZL * ZH
    zi = zh * ZL + zl
    column = []
    for k in range(1, nz):
        other = (zi + k) % nz
        column.append(((other % ZL) * NYC + yc, dy_of(other // ZL, xc, core)))
    group = [((p + k) % ndx, q) for k in range(1, ndx)]

    barrier = pltpu.get_barrier_semaphore()
    greeted = neighbours + partner + row + column + group
    for device in greeted:
        pl.semaphore_signal(barrier, inc=1, device_id=device, device_id_type=MESH)
    loads = [
        pltpu.make_async_copy(src, dst, lsem.at[n + 1])
        for n, (src, dst) in enumerate(
            [(mass_in, mass), (pot_in, pot), (conn_in, conn), (amat_in, amat), (vec_in, vec)]
        )
    ]
    for copy in loads:
        copy.start()
    load = pltpu.make_async_copy(res, rs.at[pl.ds(0, LO), pl.ds(0, 16)], lsem.at[0])
    load.start()

    def remote(src, dst, ssem, rsem, device):
        return pltpu.make_async_remote_copy(
            src_ref=src, dst_ref=dst, send_sem=ssem, recv_sem=rsem, device_id=device, device_id_type=MESH
        )

    for copy in loads[:3]:
        copy.wait()
    ct[0] = mass[...].reshape(LO * 16, EZ).T
    ct[1] = pot[...].reshape(LO * 16, EZ).T

    index = conn[0, 0]
    cell = lax.broadcasted_iota(jnp.int32, index.shape, 0)
    k = index & 15
    t = index >> 4
    i = (t * 241) >> 12
    j = t - i * EY - 8 * (cell >> 1)
    inside = (k >> 3) == (cell & 1)
    plane = jnp.where(j < 8, 648 + i * 8 + j, 720 + i)
    where = jnp.where(inside, (i * 9 + j) * 8 + (k & 7), plane)
    posr[...] = jnp.full(posr.shape, -1, jnp.int32)
    nc = index.shape[1]
    for c in range(NCELL):
        posr[c, :, 0:nc] = where[c : c + 1]
    ap[...] = jnp.zeros_like(ap)

    def spread(tile, lane):
        return jnp.broadcast_to(tile[:, lane : lane + 1], (EZ, W))

    def coefs(i, j, mass_ij, pot_ij):
        im[i, j] = mass_ij
        bt[i, j] = (pot_ij - center_shift) * (1.0 / half_width)

    for i in range(LO):
        for j in range(16):
            coefs(i, j, spread(ct[0], i * 16 + j), spread(ct[1], i * 16 + j))

    for copy in loads[3:]:
        copy.wait()
    ap[0:nc, 0:nc] = amat[...]

    def permute(c, carry):
        onehot = (lax.broadcasted_iota(jnp.int32, (KP, KP), 0) == posr[c]).astype(F32).astype(BF16)
        rows = jnp.dot(onehot, ap[...], preferred_element_type=F32).astype(BF16)
        for col in range(KP // 256):
            at = slice(col * 256, (col + 1) * 256)
            upper = lax.dot_general(
                rows[: (col + 1) * 256], onehot[at], (((1,), (1,)), ((), ())), preferred_element_type=F32
            ).astype(BF16)
            ac[c, 0 : (col + 1) * 256, at] = upper
            for line in range(col):
                ac[c, at, line * 256 : (line + 1) * 256] = upper[line * 256 : (line + 1) * 256].T
        return carry

    lax.fori_loop(0, 1, permute, 0)

    pl.semaphore_wait(barrier, len(greeted))
    halo = [
        remote(ct, cd, hs_sem.at[5], hr_sem.at[5], (pm, qm)),
        remote(vec.at[:, 0, 0], dh, hs_sem.at[2], hr_sem.at[2], (pm, qm)),
        remote(ct, cx, hs_sem.at[3], hr_sem.at[3], (pm, q)),
        remote(ct, cy_, hs_sem.at[4], hr_sem.at[4], (p, qm)),
        remote(vec.at[:, 0], xh, hs_sem.at[0], hr_sem.at[0], (pm, q)),
        remote(vec.at[:, :, 0], yh, hs_sem.at[1], hr_sem.at[1], (p, qm)),
    ]
    for copy in halo:
        copy.start()
    rhalo = [
        remote(res.at[:, 0], rs.at[pl.ds(0, LO), 16], hs_sem.at[7], hr_sem.at[7], (p, qm)),
        remote(res.at[0, pl.ds(0, 8)], rs.at[LO, pl.ds(0, 8)], hs_sem.at[6], hr_sem.at[6], (pm, q)),
        remote(res.at[0, 0], rs.at[LO, 16], hs_sem.at[8], hr_sem.at[8], (pm, qm)),
        remote(res.at[0, pl.ds(8, 8)], rs.at[LO, pl.ds(8, 8)], hs_sem.at[9], hr_sem.at[9], (pm, q)),
    ]
    for copy in rhalo[:2]:
        copy.start()

    def fill(i, carry):
        for b in range(BLOCKS):
            value = vec[b, i].astype(F32)
            y[0, b, i, 0:16] = value
            uf[b, i, 0:16] = value * im[i, 0:16]
        return carry

    lax.fori_loop(0, LO, fill, 0)
    tail = EX * 256
    rt[:, tail:] = jnp.zeros((rt.shape[0], 256), BF16)
    for b in range(BLOCKS):
        vb[b, tail:] = jnp.zeros((256, W), BF16)
    lax.fori_loop(1, NCELL, permute, 0)

    for copy in halo:
        copy.wait()
    for j in range(16):
        coefs(LO, j, spread(cx[0], j), spread(cx[1], j))
    for i in range(LO):
        coefs(i, 16, spread(cy_[0], i * 16), spread(cy_[1], i * 16))
    coefs(LO, 16, spread(cd[0], 0), spread(cd[1], 0))
    for b in range(BLOCKS):
        value = xh[b].astype(F32)
        y[0, b, LO, 0:16] = value
        uf[b, LO, 0:16] = value * im[LO, 0:16]
        value = yh[b].astype(F32)
        y[0, b, 0:LO, 16] = value
        uf[b, 0:LO, 16] = value * im[0:LO, 16]
        value = dh[b].astype(F32)
        y[0, b, LO, 16] = value
        uf[b, LO, 16] = value * im[LO, 16]

    def exchange(d, b):
        plan = [
            (sx.at[d, 1, b, 16], rd.at[d, 0, b], (pp, qp)),
            (sx.at[d, 0, b, 0], rd.at[d, 3, b], (pm, qm)),
            (sx.at[d, 0, b, 16], rd.at[d, 2, b], (pm, qp)),
            (sx.at[d, 1, b, 0], rd.at[d, 1, b], (pp, qm)),
            (sy.at[d, 1, b], ry.at[d, 0, b], (p, qp)),
            (sy.at[d, 0, b], ry.at[d, 1, b], (p, qm)),
            (sx.at[d, 1, b], rx.at[d, 0, b], (pp, q)),
            (sx.at[d, 0, b], rx.at[d, 1, b], (pm, q)),
        ]
        wanted = (0, 4, 6) if d == DEGREE - 1 else range(8)
        return [
            remote(s, t, es_sem.at[d, b, n], er_sem.at[d, b, n], to)
            for n, (s, t, to) in enumerate(plan)
            if n in wanted
        ]

    def cells(d, b):
        flat = uf.at[b].reshape(EX * EY * EZ, W)
        total = acc.at[b].reshape(EX * EY * EZ, W)
        for cy in range(2):
            for cz in range(2):
                c = cy * 2 + cz
                kp = (8 * cz + 8) % 16
                ks = slice(8 * cz, 8 * cz + 8)
                main = uf[b, :, 8 * cy : 8 * cy + 9, ks, :].reshape(648, W)
                planes = [flat[pl.ds((i * EY + 8 * cy) * EZ + kp, 8, EZ), :] for i in range(EX)]
                start = (8 * cy + 8) * EZ + kp
                line = flat[pl.ds(start, 8, EY * EZ), :]
                last = flat[pl.ds(start + 8 * EY * EZ, 1), :]
                first = lax.broadcasted_iota(jnp.int32, (8, W), 0) == 0
                last = jnp.where(first, jnp.broadcast_to(last, (8, W)), 0.0)
                whole = jnp.concatenate([main] + planes + [line, last, jnp.zeros((32, W), F32)], axis=0)
                ub[b, c] = whole.astype(BF16)
                w = jnp.dot(ac[c], ub[b, c], preferred_element_type=F32)
                wp[b, c] = w[648:]
                block = w[:648].reshape(EX, 9, 8, W)
                if cy == 0:
                    acc[b, :, 0:9, ks, :] = block
                else:
                    acc[b, :, 8, ks, :] += block[:, 0]
                    acc[b, :, 9:17, ks, :] = block[:, 1:]
            for cz in range(2):
                c = cy * 2 + cz
                kp = (8 * cz + 8) % 16
                for i in range(EX):
                    where = pl.ds((i * EY + 8 * cy) * EZ + kp, 8, EZ)
                    total[where, :] = total[where, :] + wp[b, c, 8 * i : 8 * i + 8]
                start = (8 * cy + 8) * EZ + kp
                where = pl.ds(start, 8, EY * EZ)
                total[where, :] = total[where, :] + wp[b, c, 72:80]
                where = pl.ds(start + 8 * EY * EZ, 1)
                total[where, :] = total[where, :] + wp[b, c, 80:81]
        sx[d, 0, b] = acc[b, 0].astype(BF16)
        sx[d, 1, b] = acc[b, LO].astype(BF16)
        sy[d, 0, b] = acc[b, :, 0].astype(BF16)
        sy[d, 1, b] = acc[b, :, 16].astype(BF16)
        for copy in exchange(d, b):
            copy.start()

    def update(d, b):
        now, later = d % 2, (d + 1) % 2

        def inner(i, carry):
            m = im[i]
            fresh = acc[b, i] * (m * (1.0 / half_width)) + bt[i] * y[now, b, i]
            if d > 0:
                fresh = 2.0 * fresh - y[later, b, i]
            y[later, b, i] = fresh
            if d < DEGREE - 1:
                uf[b, i] = fresh * m
            else:
                vb[b, pl.ds(pl.multiple_of(i * 256, 256), 256)] = fresh[0:16].reshape(256, W).astype(BF16)
                vb[b, pl.ds(pl.multiple_of(tail + i * EZ, EZ), EZ)] = fresh[16].astype(BF16)
            return carry

        lax.fori_loop(0, EX, inner, 0)

    def arrive(d, b):
        later = (d + 1) % 2
        factor = (1.0 if d == 0 else 2.0) / half_width

        def add(i, j, part):
            y[later, b, i, j] = y[later, b, i, j] + factor * im[i, j] * part.astype(F32)

        def refresh(i, j):
            uf[b, i, j] = y[later, b, i, j] * im[i, j]

        for copy in exchange(d, b):
            copy.wait()
        if d == DEGREE - 1:
            add(0, slice(0, 16), rx[d, 0, b, 0:16])
            add(slice(0, LO), 0, ry[d, 0, b, 0:LO])
            add(0, 0, rd[d, 0, b])
            return
        add(0, slice(0, 17), rx[d, 0, b])
        add(slice(0, EX), 0, ry[d, 0, b])
        add(0, 0, rd[d, 0, b])
        add(LO, slice(0, 17), rx[d, 1, b])
        add(slice(0, EX), 16, ry[d, 1, b])
        add(0, 16, rd[d, 1, b])
        add(LO, 0, rd[d, 2, b])
        add(LO, 16, rd[d, 3, b])
        refresh(0, slice(0, 17))
        refresh(LO, slice(0, 17))
        refresh(slice(1, LO), 0)
        refresh(slice(1, LO), 16)

    nres = rs.shape[-1]
    span = CORES * 16

    def turn_own():
        load.wait()
        for i in range(LO):
            rt[:, i * 256 : (i + 1) * 256] = rs[i, 0:16].reshape(256, nres).T

    def turn_halo():
        for copy in rhalo:
            copy.wait()
        rt[:, LO * 256 : EX * 256] = rs[LO, 0:16].reshape(256, nres).T
        rt[:, tail : tail + EX * EZ] = rs[:, 16].reshape(EX * EZ, nres).T

    def both(b, g):
        own = mloc[b, pl.ds(pl.multiple_of(g * span + core * 16, 16), 16), :]
        return own + m1r[b, g].astype(F32)

    def to_partner(b):
        return remote(m1s.at[b], m1r.at[b], s1.at[b], r1.at[b], partner[0])

    def to_row(b):
        return [remote(m2s.at[b, k], m2r.at[b, k], s2.at[b, k], r2.at[b, k], row[k]) for k in range(NXC - 1)]

    def first(b):
        mloc[b] = jnp.dot(rt[...], vb[b], preferred_element_type=F32) * norm_scale
        for g in range(ZH * NXC):
            where = pl.ds(pl.multiple_of(g * span + (CORES - 1 - core) * 16, 16), 16)
            m1s[b, g] = mloc[b, where, :].astype(BF16)
        to_partner(b).start()

    def second(b):
        to_partner(b).wait()
        for zv in range(ZH):
            for k in range(1, NXC):
                m2s[b, k - 1, zv] = both(b, zv * NXC + (xc + k) % NXC).astype(BF16)
        for copy in to_row(b):
            copy.start()

    for d in range(DEGREE):
        for b in range(BLOCKS):
            if d > 0:
                arrive(d - 1, b)
            if d == DEGREE - 1:
                for side in range(2):
                    y[side, b, LO] = jnp.zeros((EY, EZ, W), F32)
                    y[side, b, 0:LO, 16] = jnp.zeros((LO, EZ, W), F32)
            cells(d, b)
            if d == 0 and b == BLOCKS - 1:
                for copy in rhalo[2:]:
                    copy.start()
            if d == DEGREE - 1 and b > 0:
                second(b - 1)
            update(d, b)
            if d == DEGREE - 1:
                first(b)
        if d == 0:
            turn_own()
        if d == 1:
            turn_halo()
    second(BLOCKS - 1)
    final = DEGREE % 2
    for b in range(BLOCKS):
        arrive(DEGREE - 1, b)
    writes = [
        pltpu.make_async_copy(y.at[final, b, pl.ds(0, LO), pl.ds(0, 16)], out.at[b], osem.at[b])
        for b in range(BLOCKS)
    ]
    for copy in writes:
        copy.start()
    for b in range(BLOCKS):
        for copy in to_row(b):
            copy.wait()
        for zv in range(ZH):
            total = both(b, zv * NXC + xc)
            for k in range(NXC - 1):
                total = total + m2r[b, k, zv].astype(F32)
            for half in range(ZL):
                m3f[zv * ZL + half, :, b * W : (b + 1) * W] = total[half * 8 : half * 8 + 8]
                m3s[zv * ZL + half, :, b * W : (b + 1) * W] = total[half * 8 : half * 8 + 8].astype(BF16)
    copies = [
        remote(m3s.at[(zi + k + 1) % nz], m3r.at[k], s3.at[k], r3.at[k], column[k]) for k in range(nz - 1)
    ]
    for copy in copies:
        copy.start()
    for copy in copies:
        copy.wait()
    total = m3f[zi]
    for k in range(nz - 1):
        total = total + m3r[k].astype(F32)
    m4s[...] = total
    m4r[p] = total
    copies = [remote(m4s, m4r.at[p], s4.at[k], r4.at[k], group[k]) for k in range(ndx - 1)]
    for copy in copies:
        copy.start()
    for copy in copies:
        copy.wait()
    for half in range(ZL):
        total = m4r[half * NYC]
        for k in range(1, NYC):
            total = total + m4r[half * NYC + k]
        margin[half * 8 : half * 8 + 8, :] = total
    for copy in writes:
        copy.wait()


def body(vectors, resident, inv_mass, potential, cell_matrix, connectivity):
    total_nodes = inv_mass.size * lax.axis_size("dx") * lax.axis_size("dy")
    norm_scale = 1.0 / math.sqrt(total_nodes)
    nres = resident.shape[-1]
    ndx, ndy = ZL * NYC, ZH * NXC * CORES
    nz = ZL * ZH
    rows = 16 * ndy
    vmem = pl.BlockSpec(memory_space=pltpu.VMEM)
    dma = pltpu.SemaphoreType.DMA

    def k(*refs):
        kernel(norm_scale, *refs)

    state = (BLOCKS, EX, EY, EZ, W)
    results = pl.pallas_call(
        k,
        out_shape=(
            jax.ShapeDtypeStruct((BLOCKS, LO, 16, EZ, W), F32),
            jax.ShapeDtypeStruct((16, BLOCKS * W), F32),
        ),
        in_specs=[pl.BlockSpec(memory_space=pltpu.HBM)] * 6,
        out_specs=(pl.BlockSpec(memory_space=pl.ANY), vmem),
        scratch_shapes=[
            pltpu.VMEM(vectors.shape, BF16),
            pltpu.VMEM(inv_mass.shape, F32),
            pltpu.VMEM(potential.shape, F32),
            pltpu.VMEM(cell_matrix.shape, BF16),
            pltpu.VMEM(connectivity.shape, jnp.int32),
            pltpu.VMEM((KP, KP), BF16),
            pltpu.VMEM((NCELL, KP, KP), BF16),
            pltpu.VMEM(state, F32),
            pltpu.VMEM(state, F32),
            pltpu.VMEM((2, *state), F32),
            pltpu.VMEM((EX, EY, EZ, W), F32),
            pltpu.VMEM((EX, EY, EZ, W), F32),
            pltpu.VMEM((BLOCKS, NCELL, KP, W), BF16),
            pltpu.VMEM((BLOCKS, NCELL, KP - 648, W), F32),
            pltpu.VMEM((BLOCKS, rows, W), F32),
            pltpu.VMEM((EX, EY, EZ, nres), BF16),
            pltpu.VMEM((nres, (EX + 1) * 256), BF16),
            pltpu.VMEM((BLOCKS, (EX + 1) * 256, W), BF16),
            pltpu.VMEM((NCELL, 1, KP), jnp.int32),
            pltpu.VMEM((2, EZ, LO * 16), F32),
            pltpu.VMEM((BLOCKS, 16, EZ, W), BF16),
            pltpu.VMEM((BLOCKS, LO, EZ, W), BF16),
            pltpu.VMEM((BLOCKS, EZ, W), BF16),
            pltpu.VMEM((2, EZ, LO * 16), F32),
            pltpu.VMEM((2, EZ, LO * 16), F32),
            pltpu.VMEM((2, EZ, LO * 16), F32),
            pltpu.VMEM((DEGREE, 2, BLOCKS, EY, EZ, W), BF16),
            pltpu.VMEM((DEGREE, 2, BLOCKS, EX, EZ, W), BF16),
            pltpu.VMEM((DEGREE, 2, BLOCKS, EY, EZ, W), BF16),
            pltpu.VMEM((DEGREE, 2, BLOCKS, EX, EZ, W), BF16),
            pltpu.VMEM((DEGREE, 4, BLOCKS, EZ, W), BF16),
            pltpu.VMEM((BLOCKS, ZH * NXC, 16, W), BF16),
            pltpu.VMEM((BLOCKS, ZH * NXC, 16, W), BF16),
            pltpu.VMEM((BLOCKS, NXC - 1, ZH, 16, W), BF16),
            pltpu.VMEM((BLOCKS, NXC - 1, ZH, 16, W), BF16),
            pltpu.VMEM((nz, 8, BLOCKS * W), F32),
            pltpu.VMEM((nz, 8, BLOCKS * W), BF16),
            pltpu.VMEM((nz - 1, 8, BLOCKS * W), BF16),
            pltpu.VMEM((8, BLOCKS * W), F32),
            pltpu.VMEM((ndx, 8, BLOCKS * W), F32),
            dma((10,)), dma((10,)), dma((DEGREE, BLOCKS, 8)), dma((DEGREE, BLOCKS, 8)),
            dma((BLOCKS,)), dma((BLOCKS,)), dma((BLOCKS, NXC - 1)), dma((BLOCKS, NXC - 1)),
            dma((nz - 1,)), dma((nz - 1,)), dma((ndx - 1,)), dma((ndx - 1,)), dma((BLOCKS,)), dma((6,)),
        ],
        compiler_params=pltpu.CompilerParams(
            collective_id=0, has_side_effects=True, vmem_limit_bytes=62914560
        ),
    )(vectors, resident, inv_mass, potential, cell_matrix, connectivity)
    in_hbm = pl.BlockSpec(memory_space=pltpu.HBM)
    return pl.pallas_call(
        hand_on,
        out_shape=tuple(jax.ShapeDtypeStruct(r.shape, F32) for r in results),
        in_specs=[in_hbm] * 2,
        out_specs=(in_hbm, in_hbm),
        scratch_shapes=[pltpu.VMEM(r.shape, F32) for r in results] + [dma((PIECES + 1,)), dma((PIECES + 1,))],
        compiler_params=pltpu.CompilerParams(vmem_limit_bytes=60 * 1024 * 1024),
    )(*results)


PIECES = 8


def hand_on(values, rows, values_out, rows_out, held, held_rows, isem, osem):
    plan = [(rows, held_rows, rows_out)]
    step = BLOCKS * LO // PIECES
    for n in range(PIECES):
        at = (n * step // LO, pl.ds(n * step % LO, step))
        plan.append((values.at[at], held.at[at], values_out.at[at]))
    copies = []
    for n, (src, mid, dst) in enumerate(plan):
        copies.append((pltpu.make_async_copy(src, mid, isem.at[n]), pltpu.make_async_copy(mid, dst, osem.at[n])))
    for into, _ in copies:
        into.start()
    for into, back in copies:
        into.wait()
        back.start()
    for _, back in copies:
        back.wait()


def solution(mesh):
    return jax.shard_map(
        body,
        mesh=mesh,
        in_specs=(
            P(None, "dx", "dy", None, None),
            P("dx", "dy", None, None),
            P("dx", "dy", None),
            P("dx", "dy", None),
            P(),
            P("dx", "dy", None, None),
        ),
        out_specs=(P(None, "dx", "dy", None, None), P("dy", None)),
        check_vma=False,
    )
```

```python
import math

import jax
import jax.numpy as jnp
from jax import lax
from jax.experimental import pallas as pl
from jax.experimental.pallas import tpu as pltpu
from jax.sharding import PartitionSpec as P

MESH = pl.DeviceIdType.MESH
BLOCKS = 2
DEGREE = 3
NCELL = 4
KP = 768
LO, EX, EY, EZ = 8, 9, 17, 16
W = 128
center_shift = 1.2
half_width = 2.0
ZL, NYC = 2, 4
ZH, NXC, CORES = 4, 4, 2
F32, BF16 = jnp.float32, jnp.bfloat16


def kernel(
    norm_scale, vec_in, res, mass_in, pot_in, amat_in, conn_in, out, margin,
    vec, mass, pot, amat, conn,
    ap, ac, cl, sd, acc, uf, y, im, bt, ub, wp, mloc, rs, rt, vb, posr, ct,
    xh, yh, dh, cx, cy_, cd, sx, sy, rx, ry, rd,
    m1s, m1r, m2s, m2r, m3s, m3r, m4s, m4r,
    hs_sem, hr_sem, es_sem, er_sem, s1, r1, s2, r2, s3, r3, s4, r4, osem, lsem,
):
    p = lax.axis_index("dx")
    q = lax.axis_index("dy")
    ndx, ndy = ZL * NYC, ZH * NXC * CORES
    zl, yc = p // NYC, p % NYC
    core, xc, zh = q % CORES, (q // CORES) % NXC, q // (CORES * NXC)
    pm, pp = (p + ndx - 1) % ndx, (p + 1) % ndx
    qm, qp = (q + ndy - 1) % ndy, (q + 1) % ndy

    def dy_of(zhv, xv, cv):
        return (zhv * NXC + xv) * CORES + cv

    neighbours = [(pm, q), (pp, q), (p, qm), (p, qp), (pm, qm), (pp, qp), (pm, qp), (pp, qm)]
    partner = [(p, dy_of(zh, xc, CORES - 1 - core))]
    row = [(p, dy_of(zh, (xc + k) % NXC, core)) for k in range(1, NXC)]
    nz = ZL * ZH
    zi = zh * ZL + zl
    column = []
    for k in range(1, nz):
        other = (zi + k) % nz
        column.append(((other % ZL) * NYC + yc, dy_of(other // ZL, xc, core)))
    group = [((p + k) % ndx, q) for k in range(1, ndx)]

    barrier = pltpu.get_barrier_semaphore()
    greeted = neighbours + partner + row + column + group
    for device in greeted:
        pl.semaphore_signal(barrier, inc=1, device_id=device, device_id_type=MESH)
    loads = [
        pltpu.make_async_copy(src, dst, lsem.at[n + 1])
        for n, (src, dst) in enumerate(
            [(mass_in, mass), (pot_in, pot), (conn_in, conn), (amat_in, amat), (vec_in, vec)]
        )
    ]
    for copy in loads:
        copy.start()
    load = pltpu.make_async_copy(res, rs.at[pl.ds(0, LO), pl.ds(0, 16)], lsem.at[0])
    load.start()

    def remote(src, dst, ssem, rsem, device):
        return pltpu.make_async_remote_copy(
            src_ref=src, dst_ref=dst, send_sem=ssem, recv_sem=rsem, device_id=device, device_id_type=MESH
        )

    for copy in loads[:3]:
        copy.wait()
    ct[0] = mass[...].reshape(LO * 16, EZ).T
    ct[1] = pot[...].reshape(LO * 16, EZ).T

    index = conn[0, 0]
    cell = lax.broadcasted_iota(jnp.int32, index.shape, 0)
    k = index & 15
    t = index >> 4
    i = (t * 241) >> 12
    j = t - i * EY - 8 * (cell >> 1)
    inside = (k >> 3) == (cell & 1)
    plane = jnp.where(j < 8, 648 + i * 8 + j, 720 + i)
    where = jnp.where(inside, (i * 9 + j) * 8 + (k & 7), plane)
    posr[...] = jnp.full(posr.shape, -1, jnp.int32)
    nc = index.shape[1]
    for c in range(NCELL):
        posr[c, :, 0:nc] = where[c : c + 1]
    ap[...] = jnp.zeros_like(ap)

    def spread(tile, lane):
        return jnp.broadcast_to(tile[:, lane : lane + 1], (EZ, W))

    def coefs(i, j, mass_ij, pot_ij):
        im[i, j] = mass_ij
        bt[i, j] = (pot_ij - center_shift) * (1.0 / half_width)

    for i in range(LO):
        for j in range(16):
            coefs(i, j, spread(ct[0], i * 16 + j), spread(ct[1], i * 16 + j))

    for copy in loads[3:]:
        copy.wait()
    ap[0:nc, 0:nc] = amat[...]

    def permute(c, carry):
        onehot = (lax.broadcasted_iota(jnp.int32, (KP, KP), 0) == posr[c]).astype(F32).astype(BF16)
        rows = jnp.dot(onehot, ap[...], preferred_element_type=F32).astype(BF16)
        for col in range(KP // 256):
            at = slice(col * 256, (col + 1) * 256)
            upper = lax.dot_general(
                rows[: (col + 1) * 256], onehot[at], (((1,), (1,)), ((), ())), preferred_element_type=F32
            ).astype(BF16)
            ac[c, 0 : (col + 1) * 256, at] = upper
            for line in range(col):
                ac[c, at, line * 256 : (line + 1) * 256] = upper[line * 256 : (line + 1) * 256].T
        return carry

    lax.fori_loop(0, 1, permute, 0)

    pl.semaphore_wait(barrier, len(greeted))
    halo = [
        remote(ct, cd, hs_sem.at[5], hr_sem.at[5], (pm, qm)),
        remote(vec.at[:, 0, 0], dh, hs_sem.at[2], hr_sem.at[2], (pm, qm)),
        remote(ct, cx, hs_sem.at[3], hr_sem.at[3], (pm, q)),
        remote(ct, cy_, hs_sem.at[4], hr_sem.at[4], (p, qm)),
        remote(vec.at[:, 0], xh, hs_sem.at[0], hr_sem.at[0], (pm, q)),
        remote(vec.at[:, :, 0], yh, hs_sem.at[1], hr_sem.at[1], (p, qm)),
    ]
    for copy in halo:
        copy.start()
    rhalo = [
        remote(res.at[:, 0], rs.at[pl.ds(0, LO), 16], hs_sem.at[7], hr_sem.at[7], (p, qm)),
        remote(res.at[0, pl.ds(0, 8)], rs.at[LO, pl.ds(0, 8)], hs_sem.at[6], hr_sem.at[6], (pm, q)),
        remote(res.at[0, 0], rs.at[LO, 16], hs_sem.at[8], hr_sem.at[8], (pm, qm)),
        remote(res.at[0, pl.ds(8, 8)], rs.at[LO, pl.ds(8, 8)], hs_sem.at[9], hr_sem.at[9], (pm, q)),
    ]
    for copy in rhalo[:2]:
        copy.start()

    def fill(i, carry):
        for b in range(BLOCKS):
            value = vec[b, i].astype(F32)
            y[0, b, i, 0:16] = value
            uf[b, i, 0:16] = value * im[i, 0:16]
        return carry

    lax.fori_loop(0, LO, fill, 0)
    tail = EX * 256
    rt[:, tail:] = jnp.zeros((rt.shape[0], 256), BF16)
    for b in range(BLOCKS):
        vb[b, tail:] = jnp.zeros((256, W), BF16)
    lax.fori_loop(1, NCELL, permute, 0)
    for c in range(NCELL):
        jo = 8 * (c // 2)
        tops = [jo * 8, (72 + jo) * 8] + ([648, 648 + 64] if jo == 0 else [720, 728])
        for n, top in enumerate(tops):
            cl[c, 8 * n : 8 * n + 8] = ac[c, top : top + 8]

    for copy in halo:
        copy.wait()
    for j in range(16):
        coefs(LO, j, spread(cx[0], j), spread(cx[1], j))
    for i in range(LO):
        coefs(i, 16, spread(cy_[0], i * 16), spread(cy_[1], i * 16))
    coefs(LO, 16, spread(cd[0], 0), spread(cd[1], 0))
    for b in range(BLOCKS):
        value = xh[b].astype(F32)
        y[0, b, LO, 0:16] = value
        uf[b, LO, 0:16] = value * im[LO, 0:16]
        value = yh[b].astype(F32)
        y[0, b, 0:LO, 16] = value
        uf[b, 0:LO, 16] = value * im[0:LO, 16]
        value = dh[b].astype(F32)
        y[0, b, LO, 16] = value
        uf[b, LO, 16] = value * im[LO, 16]

    def exchange(d, b):
        plan = [
            (sd.at[d, 3, b], rd.at[d, 0, b], (pp, qp)),
            (sd.at[d, 0, b], rd.at[d, 3, b], (pm, qm)),
            (sd.at[d, 1, b], rd.at[d, 2, b], (pm, qp)),
            (sd.at[d, 2, b], rd.at[d, 1, b], (pp, qm)),
            (sy.at[d, 1, b], ry.at[d, 0, b], (p, qp)),
            (sy.at[d, 0, b], ry.at[d, 1, b], (p, qm)),
            (sx.at[d, 1, b], rx.at[d, 0, b], (pp, q)),
            (sx.at[d, 0, b], rx.at[d, 1, b], (pm, q)),
        ]
        wanted = (0, 4, 6) if d == DEGREE - 1 else range(8)
        return [
            remote(s, t, es_sem.at[d, b, n], er_sem.at[d, b, n], to)
            for n, (s, t, to) in enumerate(plan)
            if n in wanted
        ]

    def cells(d, b):
        flat = uf.at[b].reshape(EX * EY * EZ, W)
        total = acc.at[b].reshape(EX * EY * EZ, W)
        for cy in range(2):
            for cz in range(2):
                c = cy * 2 + cz
                kp = (8 * cz + 8) % 16
                ks = slice(8 * cz, 8 * cz + 8)
                main = uf[b, :, 8 * cy : 8 * cy + 9, ks, :].reshape(648, W)
                planes = [flat[pl.ds((i * EY + 8 * cy) * EZ + kp, 8, EZ), :] for i in range(EX)]
                start = (8 * cy + 8) * EZ + kp
                line = flat[pl.ds(start, 8, EY * EZ), :]
                last = flat[pl.ds(start + 8 * EY * EZ, 1), :]
                first = lax.broadcasted_iota(jnp.int32, (8, W), 0) == 0
                last = jnp.where(first, jnp.broadcast_to(last, (8, W)), 0.0)
                whole = jnp.concatenate([main] + planes + [line, last, jnp.zeros((32, W), F32)], axis=0)
                ub[b, c] = whole.astype(BF16)
            ends = [jnp.dot(cl[cy * 2 + cz], ub[b, cy * 2 + cz], preferred_element_type=F32) for cz in range(2)]
            place = lax.broadcasted_iota(jnp.int32, (EZ, W), 0)
            for side in range(2):
                edge = jnp.concatenate([e[8 * side : 8 * side + 8] for e in ends], axis=0)
                at8 = jnp.broadcast_to(ends[0][16 + 8 * side : 17 + 8 * side], (EZ, W))
                at0 = jnp.broadcast_to(ends[1][16 + 8 * side : 17 + 8 * side], (EZ, W))
                edge = edge + jnp.where(place == 8, at8, 0.0) + jnp.where(place == 0, at0, 0.0)
                sd[d, 2 * side + cy, b] = edge.astype(BF16)
        copies = exchange(d, b)
        far = 1 if d == DEGREE - 1 else 4
        for copy in copies[:far]:
            copy.start()
        for cy in range(2):
            for cz in range(2):
                c = cy * 2 + cz
                ks = slice(8 * cz, 8 * cz + 8)
                w = jnp.dot(ac[c], ub[b, c], preferred_element_type=F32)
                wp[b, c] = w[648:]
                block = w[:648].reshape(EX, 9, 8, W)
                if cy == 0:
                    acc[b, :, 0:9, ks, :] = block
                else:
                    acc[b, :, 8, ks, :] += block[:, 0]
                    acc[b, :, 9:17, ks, :] = block[:, 1:]
            for cz in range(2):
                c = cy * 2 + cz
                kp = (8 * cz + 8) % 16
                for i in range(EX):
                    where = pl.ds((i * EY + 8 * cy) * EZ + kp, 8, EZ)
                    total[where, :] = total[where, :] + wp[b, c, 8 * i : 8 * i + 8]
                start = (8 * cy + 8) * EZ + kp
                where = pl.ds(start, 8, EY * EZ)
                total[where, :] = total[where, :] + wp[b, c, 72:80]
                where = pl.ds(start + 8 * EY * EZ, 1)
                total[where, :] = total[where, :] + wp[b, c, 80:81]
        sx[d, 0, b] = acc[b, 0].astype(BF16)
        sx[d, 1, b] = acc[b, LO].astype(BF16)
        sy[d, 0, b] = acc[b, :, 0].astype(BF16)
        sy[d, 1, b] = acc[b, :, 16].astype(BF16)
        for copy in copies[far:]:
            copy.start()

    def update(d, b):
        now, later = d % 2, (d + 1) % 2

        def inner(i, carry):
            m = im[i]
            fresh = acc[b, i] * (m * (1.0 / half_width)) + bt[i] * y[now, b, i]
            if d > 0:
                fresh = 2.0 * fresh - y[later, b, i]
            y[later, b, i] = fresh
            if d < DEGREE - 1:
                uf[b, i] = fresh * m
            else:
                vb[b, pl.ds(pl.multiple_of(i * 256, 256), 256)] = fresh[0:16].reshape(256, W).astype(BF16)
                vb[b, pl.ds(pl.multiple_of(tail + i * EZ, EZ), EZ)] = fresh[16].astype(BF16)
            return carry

        lax.fori_loop(0, EX, inner, 0)

    def arrive(d, b):
        later = (d + 1) % 2
        factor = (1.0 if d == 0 else 2.0) / half_width

        def add(i, j, part):
            y[later, b, i, j] = y[later, b, i, j] + factor * im[i, j] * part.astype(F32)

        def refresh(i, j):
            uf[b, i, j] = y[later, b, i, j] * im[i, j]

        for copy in exchange(d, b):
            copy.wait()
        if d == DEGREE - 1:
            add(0, slice(0, 16), rx[d, 0, b, 0:16])
            add(slice(0, LO), 0, ry[d, 0, b, 0:LO])
            add(0, 0, rd[d, 0, b])
            return
        add(0, slice(0, 17), rx[d, 0, b])
        add(slice(0, EX), 0, ry[d, 0, b])
        add(0, 0, rd[d, 0, b])
        add(LO, slice(0, 17), rx[d, 1, b])
        add(slice(0, EX), 16, ry[d, 1, b])
        add(0, 16, rd[d, 1, b])
        add(LO, 0, rd[d, 2, b])
        add(LO, 16, rd[d, 3, b])
        refresh(0, slice(0, 17))
        refresh(LO, slice(0, 17))
        refresh(slice(1, LO), 0)
        refresh(slice(1, LO), 16)

    nres = rs.shape[-1]
    span = CORES * 16

    def turn_own():
        load.wait()
        for i in range(LO):
            rt[:, i * 256 : (i + 1) * 256] = rs[i, 0:16].reshape(256, nres).T

    def turn_halo():
        for copy in rhalo:
            copy.wait()
        rt[:, LO * 256 : EX * 256] = rs[LO, 0:16].reshape(256, nres).T
        rt[:, tail : tail + EX * EZ] = rs[:, 16].reshape(EX * EZ, nres).T

    def both(b, g):
        own = mloc[b, pl.ds(pl.multiple_of(g * span + core * 16, 16), 16), :]
        return own + m1r[b, g].astype(F32)

    def to_partner(b):
        return remote(m1s.at[b], m1r.at[b], s1.at[b], r1.at[b], partner[0])

    def to_row(b):
        return [remote(m2s.at[b, k], m2r.at[b, k], s2.at[b, k], r2.at[b, k], row[k]) for k in range(NXC - 1)]

    def first(b):
        mloc[b] = jnp.dot(rt[...], vb[b], preferred_element_type=F32) * norm_scale
        for g in range(ZH * NXC):
            where = pl.ds(pl.multiple_of(g * span + (CORES - 1 - core) * 16, 16), 16)
            m1s[b, g] = mloc[b, where, :].astype(BF16)
        to_partner(b).start()

    def second(b):
        to_partner(b).wait()
        for zv in range(ZH):
            for k in range(1, NXC):
                m2s[b, k - 1, zv] = both(b, zv * NXC + (xc + k) % NXC).astype(BF16)
        for copy in to_row(b):
            copy.start()

    for d in range(DEGREE):
        for b in range(BLOCKS):
            if d > 0:
                arrive(d - 1, b)
            if d == DEGREE - 1:
                for side in range(2):
                    y[side, b, LO] = jnp.zeros((EY, EZ, W), F32)
                    y[side, b, 0:LO, 16] = jnp.zeros((LO, EZ, W), F32)
            cells(d, b)
            if d == 0 and b == BLOCKS - 1:
                for copy in rhalo[2:]:
                    copy.start()
            if d == DEGREE - 1 and b > 0:
                second(b - 1)
            update(d, b)
            if d == DEGREE - 1:
                first(b)
        if d == 0:
            turn_own()
        if d == 1:
            turn_halo()
    second(BLOCKS - 1)
    final = DEGREE % 2
    for b in range(BLOCKS):
        arrive(DEGREE - 1, b)
    writes = [
        pltpu.make_async_copy(y.at[final, b, pl.ds(0, LO), pl.ds(0, 16)], out.at[b], osem.at[b])
        for b in range(BLOCKS)
    ]
    for copy in writes:
        copy.start()
    for b in range(BLOCKS):
        for copy in to_row(b):
            copy.wait()
        for zv in range(ZH):
            total = both(b, zv * NXC + xc)
            for k in range(NXC - 1):
                total = total + m2r[b, k, zv].astype(F32)
            for half in range(ZL):
                m3s[zv * ZL + half, :, b * W : (b + 1) * W] = total[half * 8 : half * 8 + 8]
    copies = [
        remote(m3s.at[(zi + k + 1) % nz], m3r.at[k], s3.at[k], r3.at[k], column[k]) for k in range(nz - 1)
    ]
    for copy in copies:
        copy.start()
    for copy in copies:
        copy.wait()
    total = m3s[zi]
    for k in range(nz - 1):
        total = total + m3r[k]
    m4s[...] = total
    m4r[p] = total
    copies = [remote(m4s, m4r.at[p], s4.at[k], r4.at[k], group[k]) for k in range(ndx - 1)]
    for copy in copies:
        copy.start()
    for copy in copies:
        copy.wait()
    for half in range(ZL):
        total = m4r[half * NYC]
        for k in range(1, NYC):
            total = total + m4r[half * NYC + k]
        margin[half * 8 : half * 8 + 8, :] = total
    for copy in writes:
        copy.wait()


def body(vectors, resident, inv_mass, potential, cell_matrix, connectivity):
    total_nodes = inv_mass.size * lax.axis_size("dx") * lax.axis_size("dy")
    norm_scale = 1.0 / math.sqrt(total_nodes)
    nres = resident.shape[-1]
    ndx, ndy = ZL * NYC, ZH * NXC * CORES
    nz = ZL * ZH
    rows = 16 * ndy
    vmem = pl.BlockSpec(memory_space=pltpu.VMEM)
    dma = pltpu.SemaphoreType.DMA

    def k(*refs):
        kernel(norm_scale, *refs)

    state = (BLOCKS, EX, EY, EZ, W)
    results = pl.pallas_call(
        k,
        out_shape=(
            jax.ShapeDtypeStruct((BLOCKS, LO, 16, EZ, W), F32),
            jax.ShapeDtypeStruct((16, BLOCKS * W), F32),
        ),
        in_specs=[pl.BlockSpec(memory_space=pltpu.HBM)] * 6,
        out_specs=(pl.BlockSpec(memory_space=pl.ANY), vmem),
        scratch_shapes=[
            pltpu.VMEM(vectors.shape, BF16),
            pltpu.VMEM(inv_mass.shape, F32),
            pltpu.VMEM(potential.shape, F32),
            pltpu.VMEM(cell_matrix.shape, BF16),
            pltpu.VMEM(connectivity.shape, jnp.int32),
            pltpu.VMEM((KP, KP), BF16),
            pltpu.VMEM((NCELL, KP, KP), BF16),
            pltpu.VMEM((NCELL, 32, KP), BF16),
            pltpu.VMEM((DEGREE, 4, BLOCKS, EZ, W), BF16),
            pltpu.VMEM(state, F32),
            pltpu.VMEM(state, F32),
            pltpu.VMEM((2, *state), F32),
            pltpu.VMEM((EX, EY, EZ, W), F32),
            pltpu.VMEM((EX, EY, EZ, W), F32),
            pltpu.VMEM((BLOCKS, NCELL, KP, W), BF16),
            pltpu.VMEM((BLOCKS, NCELL, KP - 648, W), F32),
            pltpu.VMEM((BLOCKS, rows, W), F32),
            pltpu.VMEM((EX, EY, EZ, nres), BF16),
            pltpu.VMEM((nres, (EX + 1) * 256), BF16),
            pltpu.VMEM((BLOCKS, (EX + 1) * 256, W), BF16),
            pltpu.VMEM((NCELL, 1, KP), jnp.int32),
            pltpu.VMEM((2, EZ, LO * 16), F32),
            pltpu.VMEM((BLOCKS, 16, EZ, W), BF16),
            pltpu.VMEM((BLOCKS, LO, EZ, W), BF16),
            pltpu.VMEM((BLOCKS, EZ, W), BF16),
            pltpu.VMEM((2, EZ, LO * 16), F32),
            pltpu.VMEM((2, EZ, LO * 16), F32),
            pltpu.VMEM((2, EZ, LO * 16), F32),
            pltpu.VMEM((DEGREE, 2, BLOCKS, EY, EZ, W), BF16),
            pltpu.VMEM((DEGREE, 2, BLOCKS, EX, EZ, W), BF16),
            pltpu.VMEM((DEGREE, 2, BLOCKS, EY, EZ, W), BF16),
            pltpu.VMEM((DEGREE, 2, BLOCKS, EX, EZ, W), BF16),
            pltpu.VMEM((DEGREE, 4, BLOCKS, EZ, W), BF16),
            pltpu.VMEM((BLOCKS, ZH * NXC, 16, W), BF16),
            pltpu.VMEM((BLOCKS, ZH * NXC, 16, W), BF16),
            pltpu.VMEM((BLOCKS, NXC - 1, ZH, 16, W), BF16),
            pltpu.VMEM((BLOCKS, NXC - 1, ZH, 16, W), BF16),
            pltpu.VMEM((nz, 8, BLOCKS * W), F32),
            pltpu.VMEM((nz - 1, 8, BLOCKS * W), F32),
            pltpu.VMEM((8, BLOCKS * W), F32),
            pltpu.VMEM((ndx, 8, BLOCKS * W), F32),
            dma((10,)), dma((10,)), dma((DEGREE, BLOCKS, 8)), dma((DEGREE, BLOCKS, 8)),
            dma((BLOCKS,)), dma((BLOCKS,)), dma((BLOCKS, NXC - 1)), dma((BLOCKS, NXC - 1)),
            dma((nz - 1,)), dma((nz - 1,)), dma((ndx - 1,)), dma((ndx - 1,)), dma((BLOCKS,)), dma((6,)),
        ],
        compiler_params=pltpu.CompilerParams(
            collective_id=0, has_side_effects=True, vmem_limit_bytes=62914560
        ),
    )(vectors, resident, inv_mass, potential, cell_matrix, connectivity)
    in_hbm = pl.BlockSpec(memory_space=pltpu.HBM)
    return pl.pallas_call(
        hand_on,
        out_shape=tuple(jax.ShapeDtypeStruct(r.shape, F32) for r in results),
        in_specs=[in_hbm] * 2,
        out_specs=(in_hbm, in_hbm),
        scratch_shapes=[pltpu.VMEM(r.shape, F32) for r in results] + [dma((PIECES + 1,)), dma((PIECES + 1,))],
        compiler_params=pltpu.CompilerParams(vmem_limit_bytes=60 * 1024 * 1024),
    )(*results)


PIECES = 8


def hand_on(values, rows, values_out, rows_out, held, held_rows, isem, osem):
    plan = [(rows, held_rows, rows_out)]
    step = BLOCKS * LO // PIECES
    for n in range(PIECES):
        at = (n * step // LO, pl.ds(n * step % LO, step))
        plan.append((values.at[at], held.at[at], values_out.at[at]))
    copies = []
    for n, (src, mid, dst) in enumerate(plan):
        copies.append((pltpu.make_async_copy(src, mid, isem.at[n]), pltpu.make_async_copy(mid, dst, osem.at[n])))
    for into, _ in copies:
        into.start()
    for into, back in copies:
        into.wait()
        back.start()
    for _, back in copies:
        back.wait()


def solution(mesh):
    return jax.shard_map(
        body,
        mesh=mesh,
        in_specs=(
            P(None, "dx", "dy", None, None),
            P("dx", "dy", None, None),
            P("dx", "dy", None),
            P("dx", "dy", None),
            P(),
            P("dx", "dy", None, None),
        ),
        out_specs=(P(None, "dx", "dy", None, None), P("dy", None)),
        check_vma=False,
    )
```

```python
import math

import jax
import jax.numpy as jnp
from jax import lax
from jax.experimental import pallas as pl
from jax.experimental.pallas import tpu as pltpu
from jax.sharding import PartitionSpec as P

MESH = pl.DeviceIdType.MESH
BLOCKS = 2
DEGREE = 3
NCELL = 4
KP = 768
LO, EX, EY, EZ = 8, 9, 17, 16
W = 128
center_shift = 1.2
half_width = 2.0
ZL, NYC = 2, 4
ZH, NXC, CORES = 4, 4, 2
F32, BF16 = jnp.float32, jnp.bfloat16


def kernel(
    norm_scale, vec_in, res, mass_in, pot_in, amat_in, conn_in, out, margin,
    vec, mass, pot, amat, conn,
    ap, ac, acc, uf, y, im, bt, ub, wp, mloc, rs, rt, vb, posr, ct,
    xh, yh, dh, cx, cy_, cd, sx, sy, rx, ry, rd,
    m1s, m1r, m2s, m2r, m3s, m3r, m4s, m4r,
    hs_sem, hr_sem, es_sem, er_sem, s1, r1, s2, r2, s3, r3, s4, r4, osem, lsem,
):
    p = lax.axis_index("dx")
    q = lax.axis_index("dy")
    ndx, ndy = ZL * NYC, ZH * NXC * CORES
    zl, yc = p // NYC, p % NYC
    core, xc, zh = q % CORES, (q // CORES) % NXC, q // (CORES * NXC)
    pm, pp = (p + ndx - 1) % ndx, (p + 1) % ndx
    qm, qp = (q + ndy - 1) % ndy, (q + 1) % ndy

    def dy_of(zhv, xv, cv):
        return (zhv * NXC + xv) * CORES + cv

    neighbours = [(pm, q), (pp, q), (p, qm), (p, qp), (pm, qm), (pp, qp), (pm, qp), (pp, qm)]
    partner = [(p, dy_of(zh, xc, CORES - 1 - core))]
    row = [(p, dy_of(zh, (xc + k) % NXC, core)) for k in range(1, NXC)]
    nz = ZL * ZH
    zi = zh * ZL + zl
    column = []
    for k in range(1, nz):
        other = (zi + k) % nz
        column.append(((other % ZL) * NYC + yc, dy_of(other // ZL, xc, core)))
    group = [((p + k) % ndx, q) for k in range(1, ndx)]

    barrier = pltpu.get_barrier_semaphore()
    greeted = neighbours + partner + row + column + group
    for device in greeted:
        pl.semaphore_signal(barrier, inc=1, device_id=device, device_id_type=MESH)
    loads = [
        pltpu.make_async_copy(src, dst, lsem.at[n + 1])
        for n, (src, dst) in enumerate(
            [(mass_in, mass), (pot_in, pot), (conn_in, conn), (amat_in, amat), (vec_in, vec)]
        )
    ]
    for copy in loads:
        copy.start()
    load = pltpu.make_async_copy(res, rs.at[pl.ds(0, LO), pl.ds(0, 16)], lsem.at[0])
    load.start()

    def remote(src, dst, ssem, rsem, device):
        return pltpu.make_async_remote_copy(
            src_ref=src, dst_ref=dst, send_sem=ssem, recv_sem=rsem, device_id=device, device_id_type=MESH
        )

    for copy in loads[:3]:
        copy.wait()
    ct[0] = mass[...].reshape(LO * 16, EZ).T
    ct[1] = pot[...].reshape(LO * 16, EZ).T

    index = conn[0, 0]
    cell = lax.broadcasted_iota(jnp.int32, index.shape, 0)
    k = index & 15
    t = index >> 4
    i = (t * 241) >> 12
    j = t - i * EY - 8 * (cell >> 1)
    inside = (k >> 3) == (cell & 1)
    plane = jnp.where(j < 8, 648 + i * 8 + j, 720 + i)
    where = jnp.where(inside, (i * 9 + j) * 8 + (k & 7), plane)
    posr[...] = jnp.full(posr.shape, -1, jnp.int32)
    nc = index.shape[1]
    for c in range(NCELL):
        posr[c, :, 0:nc] = where[c : c + 1]
    ap[...] = jnp.zeros_like(ap)

    def spread(tile, lane):
        return jnp.broadcast_to(tile[:, lane : lane + 1], (EZ, W))

    def coefs(i, j, mass_ij, pot_ij):
        im[i, j] = mass_ij
        bt[i, j] = (pot_ij - center_shift) * (1.0 / half_width)

    for i in range(LO):
        for j in range(16):
            coefs(i, j, spread(ct[0], i * 16 + j), spread(ct[1], i * 16 + j))

    for copy in loads[3:]:
        copy.wait()
    ap[0:nc, 0:nc] = amat[...]

    def permute(c, carry):
        onehot = (lax.broadcasted_iota(jnp.int32, (KP, KP), 0) == posr[c]).astype(F32).astype(BF16)
        rows = jnp.dot(onehot, ap[...], preferred_element_type=F32).astype(BF16)
        for col in range(KP // 256):
            at = slice(col * 256, (col + 1) * 256)
            upper = lax.dot_general(
                rows[: (col + 1) * 256], onehot[at], (((1,), (1,)), ((), ())), preferred_element_type=F32
            ).astype(BF16)
            ac[c, 0 : (col + 1) * 256, at] = upper
            for line in range(col):
                ac[c, at, line * 256 : (line + 1) * 256] = upper[line * 256 : (line + 1) * 256].T
        return carry

    lax.fori_loop(0, 1, permute, 0)

    pl.semaphore_wait(barrier, len(greeted))
    halo = [
        remote(ct, cd, hs_sem.at[5], hr_sem.at[5], (pm, qm)),
        remote(vec.at[:, 0, 0], dh, hs_sem.at[2], hr_sem.at[2], (pm, qm)),
        remote(ct, cx, hs_sem.at[3], hr_sem.at[3], (pm, q)),
        remote(ct, cy_, hs_sem.at[4], hr_sem.at[4], (p, qm)),
        remote(vec.at[:, 0], xh, hs_sem.at[0], hr_sem.at[0], (pm, q)),
        remote(vec.at[:, :, 0], yh, hs_sem.at[1], hr_sem.at[1], (p, qm)),
    ]
    for copy in halo:
        copy.start()
    rhalo = [
        remote(res.at[:, 0], rs.at[pl.ds(0, LO), 16], hs_sem.at[7], hr_sem.at[7], (p, qm)),
        remote(res.at[0, pl.ds(0, 8)], rs.at[LO, pl.ds(0, 8)], hs_sem.at[6], hr_sem.at[6], (pm, q)),
        remote(res.at[0, 0], rs.at[LO, 16], hs_sem.at[8], hr_sem.at[8], (pm, qm)),
        remote(res.at[0, pl.ds(8, 8)], rs.at[LO, pl.ds(8, 8)], hs_sem.at[9], hr_sem.at[9], (pm, q)),
    ]
    for copy in rhalo[:2]:
        copy.start()

    def fill(i, carry):
        for b in range(BLOCKS):
            value = vec[b, i].astype(F32)
            y[0, b, i, 0:16] = value
            uf[b, i, 0:16] = value * im[i, 0:16]
        return carry

    lax.fori_loop(0, LO, fill, 0)
    tail = EX * 256
    rt[:, tail:] = jnp.zeros((rt.shape[0], 256), BF16)
    for b in range(BLOCKS):
        vb[b, tail:] = jnp.zeros((256, W), BF16)
    lax.fori_loop(1, NCELL, permute, 0)

    for copy in halo:
        copy.wait()
    for j in range(16):
        coefs(LO, j, spread(cx[0], j), spread(cx[1], j))
    for i in range(LO):
        coefs(i, 16, spread(cy_[0], i * 16), spread(cy_[1], i * 16))
    coefs(LO, 16, spread(cd[0], 0), spread(cd[1], 0))
    for b in range(BLOCKS):
        value = xh[b].astype(F32)
        y[0, b, LO, 0:16] = value
        uf[b, LO, 0:16] = value * im[LO, 0:16]
        value = yh[b].astype(F32)
        y[0, b, 0:LO, 16] = value
        uf[b, 0:LO, 16] = value * im[0:LO, 16]
        value = dh[b].astype(F32)
        y[0, b, LO, 16] = value
        uf[b, LO, 16] = value * im[LO, 16]

    def exchange(d, b):
        plan = [
            (sx.at[d, 1, b, 16], rd.at[d, 0, b], (pp, qp)),
            (sx.at[d, 0, b, 0], rd.at[d, 3, b], (pm, qm)),
            (sx.at[d, 0, b, 16], rd.at[d, 2, b], (pm, qp)),
            (sx.at[d, 1, b, 0], rd.at[d, 1, b], (pp, qm)),
            (sy.at[d, 1, b], ry.at[d, 0, b], (p, qp)),
            (sy.at[d, 0, b], ry.at[d, 1, b], (p, qm)),
            (sx.at[d, 1, b], rx.at[d, 0, b], (pp, q)),
            (sx.at[d, 0, b], rx.at[d, 1, b], (pm, q)),
        ]
        wanted = (0, 4, 6) if d == DEGREE - 1 else range(8)
        return [
            remote(s, t, es_sem.at[d, b, n], er_sem.at[d, b, n], to)
            for n, (s, t, to) in enumerate(plan)
            if n in wanted
        ]

    def gather(b, c):
        cy, cz = c // 2, c % 2
        flat = uf.at[b].reshape(EX * EY * EZ, W)
        kp = (8 * cz + 8) % 16
        main = uf[b, :, 8 * cy : 8 * cy + 9, 8 * cz : 8 * cz + 8, :].reshape(648, W)
        planes = [flat[pl.ds((i * EY + 8 * cy) * EZ + kp, 8, EZ), :] for i in range(EX)]
        start = (8 * cy + 8) * EZ + kp
        line = flat[pl.ds(start, 8, EY * EZ), :]
        last = flat[pl.ds(start + 8 * EY * EZ, 1), :]
        first = lax.broadcasted_iota(jnp.int32, (8, W), 0) == 0
        last = jnp.where(first, jnp.broadcast_to(last, (8, W)), 0.0)
        whole = jnp.concatenate([main] + planes + [line, last, jnp.zeros((32, W), F32)], axis=0)
        ub[c, :, b * W : (b + 1) * W] = whole.astype(BF16)

    def place(b, c, w):
        cy, cz = c // 2, c % 2
        ks = slice(8 * cz, 8 * cz + 8)
        wp[b, c] = w[648:]
        block = w[:648].reshape(EX, 9, 8, W)
        if cy == 0:
            acc[b, :, 0:9, ks, :] = block
        else:
            acc[b, :, 8, ks, :] += block[:, 0]
            acc[b, :, 9:17, ks, :] = block[:, 1:]

    def planes_of(b, c):
        cy, cz = c // 2, c % 2
        total = acc.at[b].reshape(EX * EY * EZ, W)
        kp = (8 * cz + 8) % 16
        for i in range(EX):
            where = pl.ds((i * EY + 8 * cy) * EZ + kp, 8, EZ)
            total[where, :] = total[where, :] + wp[b, c, 8 * i : 8 * i + 8]
        start = (8 * cy + 8) * EZ + kp
        where = pl.ds(start, 8, EY * EZ)
        total[where, :] = total[where, :] + wp[b, c, 72:80]
        where = pl.ds(start + 8 * EY * EZ, 1)
        total[where, :] = total[where, :] + wp[b, c, 80:81]

    def cells(d, blocks):
        cols = slice(blocks[0] * W, (blocks[-1] + 1) * W)
        for cy in range(2):
            for cz in range(2):
                c = cy * 2 + cz
                for b in blocks:
                    gather(b, c)
                w = jnp.dot(ac[c], ub[c, :, cols], preferred_element_type=F32)
                for n, b in enumerate(blocks):
                    place(b, c, w[:, n * W : (n + 1) * W])
            for cz in range(2):
                for b in blocks:
                    planes_of(b, cy * 2 + cz)
        for b in blocks:
            sx[d, 0, b] = acc[b, 0].astype(BF16)
            sx[d, 1, b] = acc[b, LO].astype(BF16)
            sy[d, 0, b] = acc[b, :, 0].astype(BF16)
            sy[d, 1, b] = acc[b, :, 16].astype(BF16)
            for copy in exchange(d, b):
                copy.start()

    def update(d, b):
        now, later = d % 2, (d + 1) % 2

        def inner(i, carry):
            m = im[i]
            fresh = acc[b, i] * (m * (1.0 / half_width)) + bt[i] * y[now, b, i]
            if d > 0:
                fresh = 2.0 * fresh - y[later, b, i]
            y[later, b, i] = fresh
            if d < DEGREE - 1:
                uf[b, i] = fresh * m
            else:
                vb[b, pl.ds(pl.multiple_of(i * 256, 256), 256)] = fresh[0:16].reshape(256, W).astype(BF16)
                vb[b, pl.ds(pl.multiple_of(tail + i * EZ, EZ), EZ)] = fresh[16].astype(BF16)
            return carry

        lax.fori_loop(0, EX, inner, 0)

    def arrive(d, b):
        later = (d + 1) % 2
        factor = (1.0 if d == 0 else 2.0) / half_width

        def add(i, j, part):
            y[later, b, i, j] = y[later, b, i, j] + factor * im[i, j] * part.astype(F32)

        def refresh(i, j):
            uf[b, i, j] = y[later, b, i, j] * im[i, j]

        for copy in exchange(d, b):
            copy.wait()
        if d == DEGREE - 1:
            add(0, slice(0, 16), rx[d, 0, b, 0:16])
            add(slice(0, LO), 0, ry[d, 0, b, 0:LO])
            add(0, 0, rd[d, 0, b])
            return
        add(0, slice(0, 17), rx[d, 0, b])
        add(slice(0, EX), 0, ry[d, 0, b])
        add(0, 0, rd[d, 0, b])
        add(LO, slice(0, 17), rx[d, 1, b])
        add(slice(0, EX), 16, ry[d, 1, b])
        add(0, 16, rd[d, 1, b])
        add(LO, 0, rd[d, 2, b])
        add(LO, 16, rd[d, 3, b])
        refresh(0, slice(0, 17))
        refresh(LO, slice(0, 17))
        refresh(slice(1, LO), 0)
        refresh(slice(1, LO), 16)

    nres = rs.shape[-1]
    span = CORES * 16

    def turn_own():
        load.wait()
        for i in range(LO):
            rt[:, i * 256 : (i + 1) * 256] = rs[i, 0:16].reshape(256, nres).T

    def turn_halo():
        for copy in rhalo:
            copy.wait()
        rt[:, LO * 256 : EX * 256] = rs[LO, 0:16].reshape(256, nres).T
        rt[:, tail : tail + EX * EZ] = rs[:, 16].reshape(EX * EZ, nres).T

    def both(b, g):
        own = mloc[b, pl.ds(pl.multiple_of(g * span + core * 16, 16), 16), :]
        return own + m1r[b, g].astype(F32)

    def to_partner(b):
        return remote(m1s.at[b], m1r.at[b], s1.at[b], r1.at[b], partner[0])

    def to_row(b):
        return [remote(m2s.at[b, k], m2r.at[b, k], s2.at[b, k], r2.at[b, k], row[k]) for k in range(NXC - 1)]

    def first(b):
        mloc[b] = jnp.dot(rt[...], vb[b], preferred_element_type=F32) * norm_scale
        for g in range(ZH * NXC):
            where = pl.ds(pl.multiple_of(g * span + (CORES - 1 - core) * 16, 16), 16)
            m1s[b, g] = mloc[b, where, :].astype(BF16)
        to_partner(b).start()

    def second(b):
        to_partner(b).wait()
        for zv in range(ZH):
            for k in range(1, NXC):
                m2s[b, k - 1, zv] = both(b, zv * NXC + (xc + k) % NXC).astype(BF16)
        for copy in to_row(b):
            copy.start()

    for d in range(DEGREE):
        for b in range(BLOCKS):
            if d > 0:
                arrive(d - 1, b)
            if d == DEGREE - 1:
                for side in range(2):
                    y[side, b, LO] = jnp.zeros((EY, EZ, W), F32)
                    y[side, b, 0:LO, 16] = jnp.zeros((LO, EZ, W), F32)
            if d > 0:
                cells(d, (b,))
            elif b == 0:
                cells(d, tuple(range(BLOCKS)))
            if d == 0 and b == BLOCKS - 1:
                for copy in rhalo[2:]:
                    copy.start()
            if d == DEGREE - 1 and b > 0:
                second(b - 1)
            update(d, b)
            if d == DEGREE - 1:
                first(b)
        if d == 0:
            turn_own()
        if d == 1:
            turn_halo()
    second(BLOCKS - 1)
    final = DEGREE % 2
    for b in range(BLOCKS):
        arrive(DEGREE - 1, b)
    writes = [
        pltpu.make_async_copy(y.at[final, b, pl.ds(0, LO), pl.ds(0, 16)], out.at[b], osem.at[b])
        for b in range(BLOCKS)
    ]
    for copy in writes:
        copy.start()
    for b in range(BLOCKS):
        for copy in to_row(b):
            copy.wait()
        for zv in range(ZH):
            total = both(b, zv * NXC + xc)
            for k in range(NXC - 1):
                total = total + m2r[b, k, zv].astype(F32)
            for half in range(ZL):
                m3s[zv * ZL + half, :, b * W : (b + 1) * W] = total[half * 8 : half * 8 + 8]
    copies = [
        remote(m3s.at[(zi + k + 1) % nz], m3r.at[k], s3.at[k], r3.at[k], column[k]) for k in range(nz - 1)
    ]
    for copy in copies:
        copy.start()
    for copy in copies:
        copy.wait()
    total = m3s[zi]
    for k in range(nz - 1):
        total = total + m3r[k]
    m4s[...] = total
    m4r[p] = total
    copies = [remote(m4s, m4r.at[p], s4.at[k], r4.at[k], group[k]) for k in range(ndx - 1)]
    for copy in copies:
        copy.start()
    for copy in copies:
        copy.wait()
    for half in range(ZL):
        total = m4r[half * NYC]
        for k in range(1, NYC):
            total = total + m4r[half * NYC + k]
        margin[half * 8 : half * 8 + 8, :] = total
    for copy in writes:
        copy.wait()


def body(vectors, resident, inv_mass, potential, cell_matrix, connectivity):
    total_nodes = inv_mass.size * lax.axis_size("dx") * lax.axis_size("dy")
    norm_scale = 1.0 / math.sqrt(total_nodes)
    nres = resident.shape[-1]
    ndx, ndy = ZL * NYC, ZH * NXC * CORES
    nz = ZL * ZH
    rows = 16 * ndy
    vmem = pl.BlockSpec(memory_space=pltpu.VMEM)
    dma = pltpu.SemaphoreType.DMA

    def k(*refs):
        kernel(norm_scale, *refs)

    state = (BLOCKS, EX, EY, EZ, W)
    results = pl.pallas_call(
        k,
        out_shape=(
            jax.ShapeDtypeStruct((BLOCKS, LO, 16, EZ, W), F32),
            jax.ShapeDtypeStruct((16, BLOCKS * W), F32),
        ),
        in_specs=[pl.BlockSpec(memory_space=pltpu.HBM)] * 6,
        out_specs=(pl.BlockSpec(memory_space=pl.ANY), vmem),
        scratch_shapes=[
            pltpu.VMEM(vectors.shape, BF16),
            pltpu.VMEM(inv_mass.shape, F32),
            pltpu.VMEM(potential.shape, F32),
            pltpu.VMEM(cell_matrix.shape, BF16),
            pltpu.VMEM(connectivity.shape, jnp.int32),
            pltpu.VMEM((KP, KP), BF16),
            pltpu.VMEM((NCELL, KP, KP), BF16),
            pltpu.VMEM(state, F32),
            pltpu.VMEM(state, F32),
            pltpu.VMEM((2, *state), F32),
            pltpu.VMEM((EX, EY, EZ, W), F32),
            pltpu.VMEM((EX, EY, EZ, W), F32),
            pltpu.VMEM((NCELL, KP, BLOCKS * W), BF16),
            pltpu.VMEM((BLOCKS, NCELL, KP - 648, W), F32),
            pltpu.VMEM((BLOCKS, rows, W), F32),
            pltpu.VMEM((EX, EY, EZ, nres), BF16),
            pltpu.VMEM((nres, (EX + 1) * 256), BF16),
            pltpu.VMEM((BLOCKS, (EX + 1) * 256, W), BF16),
            pltpu.VMEM((NCELL, 1, KP), jnp.int32),
            pltpu.VMEM((2, EZ, LO * 16), F32),
            pltpu.VMEM((BLOCKS, 16, EZ, W), BF16),
            pltpu.VMEM((BLOCKS, LO, EZ, W), BF16),
            pltpu.VMEM((BLOCKS, EZ, W), BF16),
            pltpu.VMEM((2, EZ, LO * 16), F32),
            pltpu.VMEM((2, EZ, LO * 16), F32),
            pltpu.VMEM((2, EZ, LO * 16), F32),
            pltpu.VMEM((DEGREE, 2, BLOCKS, EY, EZ, W), BF16),
            pltpu.VMEM((DEGREE, 2, BLOCKS, EX, EZ, W), BF16),
            pltpu.VMEM((DEGREE, 2, BLOCKS, EY, EZ, W), BF16),
            pltpu.VMEM((DEGREE, 2, BLOCKS, EX, EZ, W), BF16),
            pltpu.VMEM((DEGREE, 4, BLOCKS, EZ, W), BF16),
            pltpu.VMEM((BLOCKS, ZH * NXC, 16, W), BF16),
            pltpu.VMEM((BLOCKS, ZH * NXC, 16, W), BF16),
            pltpu.VMEM((BLOCKS, NXC - 1, ZH, 16, W), BF16),
            pltpu.VMEM((BLOCKS, NXC - 1, ZH, 16, W), BF16),
            pltpu.VMEM((nz, 8, BLOCKS * W), F32),
            pltpu.VMEM((nz - 1, 8, BLOCKS * W), F32),
            pltpu.VMEM((8, BLOCKS * W), F32),
            pltpu.VMEM((ndx, 8, BLOCKS * W), F32),
            dma((10,)), dma((10,)), dma((DEGREE, BLOCKS, 8)), dma((DEGREE, BLOCKS, 8)),
            dma((BLOCKS,)), dma((BLOCKS,)), dma((BLOCKS, NXC - 1)), dma((BLOCKS, NXC - 1)),
            dma((nz - 1,)), dma((nz - 1,)), dma((ndx - 1,)), dma((ndx - 1,)), dma((BLOCKS,)), dma((6,)),
        ],
        compiler_params=pltpu.CompilerParams(
            collective_id=0, has_side_effects=True, vmem_limit_bytes=62914560
        ),
    )(vectors, resident, inv_mass, potential, cell_matrix, connectivity)
    in_hbm = pl.BlockSpec(memory_space=pltpu.HBM)
    return pl.pallas_call(
        hand_on,
        out_shape=tuple(jax.ShapeDtypeStruct(r.shape, F32) for r in results),
        in_specs=[in_hbm] * 2,
        out_specs=(in_hbm, in_hbm),
        scratch_shapes=[pltpu.VMEM(r.shape, F32) for r in results] + [dma((PIECES + 1,)), dma((PIECES + 1,))],
        compiler_params=pltpu.CompilerParams(vmem_limit_bytes=60 * 1024 * 1024),
    )(*results)


PIECES = 8


def hand_on(values, rows, values_out, rows_out, held, held_rows, isem, osem):
    plan = [(rows, held_rows, rows_out)]
    step = BLOCKS * LO // PIECES
    for n in range(PIECES):
        at = (n * step // LO, pl.ds(n * step % LO, step))
        plan.append((values.at[at], held.at[at], values_out.at[at]))
    copies = []
    for n, (src, mid, dst) in enumerate(plan):
        copies.append((pltpu.make_async_copy(src, mid, isem.at[n]), pltpu.make_async_copy(mid, dst, osem.at[n])))
    for into, _ in copies:
        into.start()
    for into, back in copies:
        into.wait()
        back.start()
    for _, back in copies:
        back.wait()


def solution(mesh):
    return jax.shard_map(
        body,
        mesh=mesh,
        in_specs=(
            P(None, "dx", "dy", None, None),
            P("dx", "dy", None, None),
            P("dx", "dy", None),
            P("dx", "dy", None),
            P(),
            P("dx", "dy", None, None),
        ),
        out_specs=(P(None, "dx", "dy", None, None), P("dy", None)),
        check_vma=False,
    )
```
